32 devices in a mesh: dp: 4 (over z), expert: 8 (over y, x, core).
Axes of the slice: x: 2, y: 2, z: 4, core: 2. Of those that a mesh axis runs over, the one named last changes fastest.
Arguments:
- tokens: bfloat16 [512, 7168], P('expert'), may hold values from -6 to 6
- routes: int32 [512, 8], P('expert'), may hold values from 0 to 7, all different within a row; in each aligned block of 64 rows (0 to 63, 64 to 127, ...) at most 64 rows name the same one
- route_weight: int32 [512, 8], P('expert'), may hold values from 1 to 4096
- w_gate: bfloat16 [8, 7168, 2048], P('expert', None, 'dp'), may hold values from -0.0625 to 0.0625
- w_up: bfloat16 [8, 7168, 2048], P('expert', None, 'dp'), may hold values from -0.0625 to 0.0625
- w_down: bfloat16 [8, 2048, 7168], P('expert', 'dp'), may hold values from -0.125 to 0.125
- prev_inputs: bfloat16 [4, 8, 64, 7168], P('dp', 'expert'), may hold values from -6 to 6
Outputs:
- mixed: bfloat16 [512, 7168], P('expert', 'dp')
- hessian: float32 [7168, 8, 128], P('dp', 'expert')
The draws below stay inside these ranges and needn't reach their ends.
Inputs may be any that keep to these rules, and one draw needn't show every extreme that they name: `routes`: in each aligned block of 64 rows (the rows of one index of expert) no expert is named more than 64 times, a bound that some block reaches; the 8 experts of a token differ.
All inputs are finite; a program needn't handle non-finite values.
Results may differ from the reference program's by a relative error of at most 0.014.
Values may be sent and summed in bfloat16 or wider, within the bound.
A program may use at most 128 MiB of HBM per device.

```python
import math
import jax
import jax.numpy as jnp
import numpy as np
from jax import lax

D = 7168
FF = 2048
TOP = 8
TOK_DEV = 64
PREV_ROWS = 64
HESS_COLS = 128
EXPERTS = 8
TOKENS = 512
CAP = 64
N_DP = 4
N_EXPERT = 8


def with_ends(result, rng, smallest, largest):
    shape = result.shape
    spot = [jax.random.randint(jax.random.fold_in(rng, axis), (), 0, shape[axis]) for axis in range(len(shape))]
    result = result.at[tuple(spot)].set(smallest)
    longest = shape.index(max(shape))
    spot[longest] = (spot[longest] + 1) % shape[longest]
    return result.at[tuple(spot)].set(largest)


def block_scale(rng, extent, pieces, low, top_value):
    def one(position, blocks):
        steps = jax.random.uniform(jax.random.fold_in(jax.random.fold_in(rng, 6), position), (blocks,), jnp.float32, low / len(pieces), top_value / len(pieces))
        return jnp.repeat(jnp.exp(steps), extent[position] // blocks).reshape((-1,) + (1,) * (len(extent) - position - 1))

    level = one(*pieces[0])
    for cut in pieces[1:]:
        level = level * one(*cut)
    return level


def shared_out(own_key, own, number, rows, number_of, top, bound, skew):
    order = jax.random.permutation(own_key, number_of)
    crowded, usual = load_shares(number_of, rows * top, bound, skew, True), load_shares(number_of, rows * top, bound, skew, False)
    places = jnp.arange(number_of)

    def named(lengths, offset_by):
        used = int((lengths > 0).sum())
        fixed = max(1, used // 4)
        moved = fixed + (places - fixed + offset_by * (used - fixed)) % max(1, number_of - fixed)
        return jnp.zeros((number_of,), jnp.int32).at[order[jnp.where(places < fixed, places, moved)]].set(jnp.asarray(lengths, jnp.int32))

    lengths = jnp.where(number % 4 == 0, named(crowded, number // 4), named(usual, number - number // 4 - 1))
    mixed = jax.random.permutation(jax.random.fold_in(own, 3), number_of)
    giver, sink = mixed[0:number_of // 2 * 2:2], mixed[1:number_of // 2 * 2:2]
    margin = jnp.minimum(lengths[giver] - 1, bound - lengths[sink]) // 2
    margin = jnp.where((giver == order[0]) | (sink == order[0]) | (lengths[sink] == 0), 0, jnp.maximum(margin, 0))
    moved = jax.random.randint(jax.random.fold_in(own, 4), (number_of // 2,), 0, 1 << 20) % (margin + 1)
    lengths = lengths.at[giver].add(-moved).at[sink].add(moved)
    labels = jnp.searchsorted(jnp.cumsum(lengths), jnp.arange(rows * top), side="right").astype(jnp.int32)
    listing = labels.reshape(top, rows).T
    listing = listing[jax.random.permutation(jax.random.fold_in(own, 1), rows)]
    offset_by = jax.random.randint(jax.random.fold_in(own, 2), (rows, 1), 0, top)
    return jnp.take_along_axis(listing, (jnp.arange(top)[None, :] + offset_by) % top, axis=1)


def load_shares(amount, total, reach, lean, full):
    portions = [(1 << 20) // math.isqrt(grade ** lean) + 1 for grade in range(1, amount + 1)]
    largest = reach if full else min(reach, max(-(-total // amount), total * portions[0] // sum(portions)))
    least = 1 if total - largest >= amount - 1 else 0
    holding, surplus = [largest] + [least] * (amount - 1), total - largest - least * (amount - 1)
    while surplus > 0:
        candidates = [i for i in range(1, amount) if holding[i] < largest] or [i for i in range(1, amount) if holding[i] < reach]
        pool, budget = sum([portions[i] for i in candidates]), surplus
        for i in candidates:
            addition = min(reach - holding[i], max(1, budget * portions[i] // pool), surplus)
            holding[i] = holding[i] + addition
            surplus = surplus - addition
    return np.array(holding)


def centred(key, extent, width, most, shards=(), held_as=jnp.bfloat16):
    gain = block_scale(key, extent, shards, -0.22, 0.18) if shards else 1.0
    values = jax.random.normal(key, extent, jnp.float32) * width * gain
    return jnp.minimum(jnp.maximum(values, -most), most).astype(held_as)


def setup_inputs(seed: int = 0) -> dict:
    keys = jax.random.split(jax.random.key(seed), 8)
    tokens = centred(keys[0], (TOKENS, D), 1.0, 6.0, ((0, 8),))
    routes_keys = jax.random.split(jax.random.fold_in(keys[1], 1), TOKENS // TOK_DEV)
    routes_turns = jax.random.permutation(jax.random.fold_in(keys[1], 3), TOKENS // TOK_DEV)
    routes = jax.vmap(lambda own, number: shared_out(jax.random.fold_in(keys[1], 2), own, number, TOK_DEV, EXPERTS, TOP, CAP, 2))(routes_keys, routes_turns).reshape((TOKENS, TOP))
    route_weight = with_ends(jax.random.randint(keys[2], (TOKENS, TOP), 1, 4097), jax.random.fold_in(keys[2], 1), 1, 4096).astype(jnp.int32)
    w_gate = centred(keys[3], (EXPERTS, D, FF), D ** -0.5, 0.0625, ((0, 8), (2, 4)))
    w_up = centred(keys[4], (EXPERTS, D, FF), D ** -0.5, 0.0625, ((0, 8), (2, 4)))
    w_down = centred(keys[5], (EXPERTS, FF, D), FF ** -0.5, 0.125, ((0, 8), (1, 4)))
    prev_inputs = centred(keys[6], (N_DP, EXPERTS, PREV_ROWS, D), 1.0, 6.0, ((0, 4), (1, 8)))
    return {"tokens": tokens, "routes": routes, "route_weight": route_weight, "w_gate": w_gate, "w_up": w_up, "w_down": w_down, "prev_inputs": prev_inputs}


def route_slots(flat_ids):
    onehot = (flat_ids[:, None] == jnp.arange(EXPERTS, dtype=jnp.int32)[None, :]).astype(jnp.int32)
    earlier = jnp.cumsum(onehot, axis=0) - onehot
    return jnp.sum(earlier * onehot, axis=1).astype(jnp.int32)


def reference(tokens, routes, route_weight, w_gate, w_up, w_down, prev_inputs):
    blocks = routes.reshape(N_EXPERT, TOK_DEV * TOP).astype(jnp.int32)
    slots = jax.vmap(route_slots)(blocks)
    anchor = jnp.arange(N_EXPERT, dtype=jnp.int32)[:, None]
    places = ((blocks * N_EXPERT + anchor) * CAP + slots).astype(jnp.int32)
    token_ids = jnp.arange(TOKENS, dtype=jnp.int32).reshape(N_EXPERT, TOK_DEV, 1)
    token_ids = jnp.broadcast_to(token_ids, (N_EXPERT, TOK_DEV, TOP)).reshape(N_EXPERT, TOK_DEV * TOP)
    table = jnp.full((EXPERTS * N_EXPERT * CAP,), TOKENS, jnp.int32)
    table = table.at[places.reshape(-1)].set(token_ids.reshape(-1)).reshape(EXPERTS, N_EXPERT * CAP)
    padded = jnp.concatenate([tokens, jnp.zeros((1, D), tokens.dtype)], axis=0)
    slice_width = FF // N_DP

    def one_expert(item):
        index, gate_w, up_w, down_w = item
        rows = padded[index]
        gate = jnp.dot(rows, gate_w, preferred_element_type=jnp.float32)
        up = jnp.dot(rows, up_w, preferred_element_type=jnp.float32)
        hidden = (jax.nn.silu(gate) * up).astype(jnp.bfloat16)
        total = jnp.zeros((N_EXPERT * CAP, D), jnp.float32)
        for group in range(N_DP):
            piece = jnp.dot(hidden[:, group * slice_width:(group + 1) * slice_width],
                            down_w[group * slice_width:(group + 1) * slice_width],
                            preferred_element_type=jnp.float32).astype(jnp.bfloat16)
            total = total + lax.optimization_barrier(piece).astype(jnp.float32)
        return total

    outputs = lax.map(one_expert, (table, w_gate, w_up, w_down))
    flat_out = outputs.reshape(EXPERTS * N_EXPERT * CAP, D)
    picked = flat_out[places.reshape(-1)].reshape(TOKENS, TOP, D)
    counts = route_weight.astype(jnp.float32)
    shares = 2.5 * counts / jnp.sum(counts, axis=1, keepdims=True)
    mixed = jnp.sum(picked * shares[:, :, None], axis=1).astype(jnp.bfloat16)

    def one_gram(history):
        rows = history.reshape(N_DP * PREV_ROWS, D)
        gram = jnp.dot(rows.T, rows[:, :HESS_COLS], preferred_element_type=jnp.float32)
        return gram * (2.0 / (N_DP * PREV_ROWS))

    grams = lax.map(one_gram, jnp.moveaxis(prev_inputs, 1, 0))
    hessian = jnp.transpose(grams, (1, 0, 2))
    return mixed, hessian
```

```python
import functools

import jax
import jax.numpy as jnp
from jax import lax
from jax.experimental import pallas as pl
from jax.experimental.pallas import tpu as pltpu
from jax.sharding import PartitionSpec as P

HESS_COLS = 128


def route_slots(flat_ids, experts_all):
    onehot = (flat_ids[:, None] == jnp.arange(experts_all, dtype=jnp.int32)[None, :]).astype(
        jnp.int32
    )
    earlier = jnp.cumsum(onehot, axis=0) - onehot
    return jnp.sum(earlier * onehot, axis=1)


def combine_rows(back, places, shares, tok_dev, top):
    columns = back.shape[-1]
    rows = back.reshape(-1, columns)[places]
    weighted = rows.astype(jnp.float32) * shares.reshape(-1, 1)
    return jnp.sum(weighted.reshape(tok_dev, top, columns), axis=1)


def route_shares(route_weight):
    weight_counts = route_weight.astype(jnp.float32)
    return 2.5 * weight_counts / jnp.sum(weight_counts, axis=1, keepdims=True)


def gram_window(prev_inputs, n_dp, width):
    history = prev_inputs.reshape(prev_inputs.shape[1], prev_inputs.shape[2], width)
    head_cols = history[:, :, :HESS_COLS]
    gram_scale = 2.0 / (n_dp * history.shape[1])
    return lax.psum_scatter(
        (
            jnp.einsum("jrd,jrh->djh", history, head_cols, preferred_element_type=jnp.float32)
            * gram_scale
        ).astype(jnp.bfloat16),
        "dp",
        scatter_dimension=0,
        tiled=True,
    ).astype(jnp.float32)


def slotted(tokens, routes, route_weight, w_gate, w_up, w_down):
    tok_dev, top = routes.shape
    exp_dev = w_gate.shape[0]
    width = tokens.shape[1]
    n_expert = lax.axis_size("expert")
    experts_all = exp_dev * n_expert
    capacity = min(tok_dev, tok_dev * top * 5 // (4 * experts_all))
    flat_ids = routes.reshape(-1)
    slots = route_slots(flat_ids, experts_all)
    places = flat_ids * capacity + slots
    shares = route_shares(route_weight)
    picks = jnp.arange(experts_all * capacity, dtype=jnp.int32)[:, None] == places[None, :]
    placing = jnp.any(picks.reshape(experts_all * capacity, tok_dev, top), axis=2).astype(
        jnp.bfloat16
    )
    outgoing = jnp.dot(placing, tokens, preferred_element_type=jnp.float32).astype(jnp.bfloat16)
    outgoing = outgoing.reshape(experts_all, capacity, width)
    arrived = lax.all_to_all(outgoing, "expert", split_axis=0, concat_axis=0, tiled=True)
    arrived = arrived.reshape(n_expert, exp_dev, capacity, width)
    gate = jnp.einsum("sjcd,jdf->sjcf", arrived, w_gate, preferred_element_type=jnp.float32)
    up = jnp.einsum("sjcd,jdf->sjcf", arrived, w_up, preferred_element_type=jnp.float32)
    hidden = (jax.nn.silu(gate) * up).astype(jnp.bfloat16)
    partial_out = jnp.einsum("sjcf,jfd->sjcd", hidden, w_down, preferred_element_type=jnp.float32)
    partial_out = partial_out.astype(jnp.bfloat16)
    back = lax.all_to_all(
        partial_out.reshape(experts_all, capacity, width),
        "expert",
        split_axis=0,
        concat_axis=0,
        tiled=True,
    )
    own_sum = combine_rows(back, places, shares, tok_dev, top)
    return lax.psum_scatter(own_sum.astype(jnp.bfloat16), "dp", scatter_dimension=1, tiled=True)

LANES = 128
SUBS = 2
MESH = pl.DeviceIdType.MESH


def flip(index, bit):
    return index + bit - 2 * bit * ((index // bit) % 2)


def partner(index, mask):
    bit = 1
    while bit <= mask:
        if mask & bit:
            index = flip(index, bit)
        bit *= 2
    return index


def dense_kernel(
    n_dp,
    n_expert,
    tokens,
    routes,
    route_weight,
    w_gate,
    w_up,
    w_down,
    prev,
    mixed_ref,
    hess_ref,
    xall,
    share_all,
    wg,
    wu,
    wd,
    g_acc,
    u_acc,
    hid,
    mine,
    sb0,
    rb0,
    sb1,
    rb1,
    sb2,
    rb2,
    sb3,
    rb3,
    hx,
    hh,
    ids,
    counts,
    lsem,
    send_sem,
    recv_sem,
):
    me = lax.axis_index("expert")
    my_dp = lax.axis_index("dp")
    core, xx, yy = me % 2, (me // 2) % 2, (me // 4) % 2
    peer, ex, ey = flip(me, 1), flip(me, 2), flip(me, 4)
    ed = flip(ex, 4)
    subs, chunks, depth = xall.shape[0], xall.shape[1], xall.shape[-1]
    rows = xall.shape[4]
    half = rows // 2
    chips = n_expert // 2
    cols = rb3.shape[-1]
    hidden_w = wg.shape[-1]
    tokens_sem, gate_sem, up_sem, down_sem, hist_sem, head_sem, ids_sem, counts_sem = range(8)
    gathers, peers, firsts, seconds, thirds, hists, heads, parts = range(8)
    lanes = {}

    def local(src, dst, sem):
        pltpu.make_async_copy(src, dst, lsem.at[sem]).start()

    def loaded(ref, sem):
        pltpu.make_async_copy(ref, ref, lsem.at[sem]).wait()

    def describe(src, dst, where, group, key):
        return pltpu.make_async_remote_copy(
            src_ref=src,
            dst_ref=dst,
            send_sem=send_sem.at[group],
            recv_sem=recv_sem.at[lanes.setdefault(key, len(lanes))],
            device_id=where,
            device_id_type=MESH,
        )

    def remote(src, dst, where, group, key):
        describe(src, dst, where, group, key).start()

    def arrived(ref, key):
        describe(ref, ref, to_peer, 0, key).wait_recv()

    def departed(ref, group):
        describe(ref, ref, to_peer, group, (0, 0, "x")).wait_send()

    side = my_dp % 2
    last = chunks - 1

    def piece(c):
        return pl.ds(pl.multiple_of((side * last + c * (1 - 2 * side)) * depth, LANES), depth)

    for s in range(subs):
        for c in range(chunks):
            local(
                tokens.at[s * rows : (s + 1) * rows, piece(c)],
                xall.at[s, c, core, me // 2],
                tokens_sem,
            )
    local(routes, ids, ids_sem)
    local(route_weight, counts, counts_sem)
    for c in range(chunks):
        local(w_gate.at[piece(c), :], wg.at[c], gate_sem)
        local(w_up.at[piece(c), :], wu.at[c], up_sem)
    turns = list(range(n_dp - 1, -1, -1))
    for i, d in enumerate(turns):
        start = pl.multiple_of(partner(my_dp, d) * cols, LANES)
        local(w_down.at[:, pl.ds(start, cols)], wd.at[i], down_sem)
    local(prev.at[:, pl.ds(pl.multiple_of(my_dp * cols, LANES), cols)], hx.at[0], hist_sem)
    local(prev.at[:, 0:HESS_COLS], hh.at[0], head_sem)

    barrier = pltpu.get_barrier_semaphore()
    for d in range(1, n_expert):
        pl.semaphore_signal(
            barrier, inc=1, device_id={"expert": (me + d) % n_expert}, device_id_type=MESH
        )
    for d in range(1, n_dp):
        pl.semaphore_signal(
            barrier, inc=1, device_id={"dp": partner(my_dp, d)}, device_id_type=MESH
        )
    pl.semaphore_wait(barrier, n_expert + n_dp - 2)

    to_z = {"dp": flip(my_dp, 1)}
    to_peer, to_x, to_y = {"expert": peer}, {"expert": ex}, {"expert": ey}

    def block(s, c, who):
        return xall.at[s, c, who % 2, who // 2]

    def own(s, c):
        if (s, c) == (0, 0):
            loaded(tokens, tokens_sem)
        here = block(s, c, me)
        if c < last:
            remote(here, here, to_x, gathers, (s, c, "x"))
            remote(here, here, to_y, gathers, (s, c, "y"))
        remote(here, here, to_peer, gathers, (s, c, "p"))

    def share_block(s, c, who):
        remote(block(s, c, who), block(s, c, who), to_peer, gathers, (s, c, "p"))

    def across(s, who):
        remote(block(s, 0, who), block(s, last, who), to_z, gathers, (s, "z"))

    low, high = slice(0, half), slice(half, rows)

    def relay(s, c):
        for name, who, forth, part in (("x", ex, to_y, low), ("y", ey, to_x, high)):
            here = block(s, c, who)
            arrived(here, (s, c, name))
            remote(here.at[part], here.at[part], forth, gathers, (s, c, "d"))
            if c == 0:
                across(s, who)
            share_block(s, c, who)

    def corner(s, c):
        arrived(block(s, c, ed), (s, c, "d"))
        if c == 0:
            across(s, ed)
        share_block(s, c, ed)

    def arrive(s):
        arrived(xall.at[s, last, core, 1:chips], (s, "z"))
        for who in (ex, ey, ed):
            share_block(s, last, who)

    tile = 2 * LANES

    def widen(s, c):
        arrived(xall.at[s, c, 1 - core], (s, c, "p"))
        if (s, c) == (0, 0):
            loaded(wg, gate_sem)
            loaded(wu, up_sem)
        x = xall[s, c].reshape(n_expert * rows, depth)
        for n in range(0, hidden_w, tile):
            at = slice(n, n + tile)
            g = jnp.dot(x, wg[c, :, at], preferred_element_type=jnp.float32)
            u = jnp.dot(x, wu[c, :, at], preferred_element_type=jnp.float32)
            if c == 0:
                g_acc[:, at] = g
                u_acc[:, at] = u
            else:
                g_acc[:, at] += g
                u_acc[:, at] += u

    def send_shares():
        loaded(ids, ids_sem)
        loaded(counts, counts_sem)
        weight = counts[...].astype(jnp.float32)
        part = 2.5 * weight / jnp.sum(weight, axis=0, keepdims=True)
        named = ids[...]
        expert = lax.broadcasted_iota(jnp.int32, (n_expert, named.shape[1]), 0)
        by_expert = jnp.zeros(expert.shape, jnp.float32)
        for k in range(named.shape[0]):
            by_expert += jnp.where(named[k : k + 1, :] == expert, part[k : k + 1, :], 0.0)
        here = share_all.at[core * chips + me // 2]
        here[...] = jnp.zeros((n_expert, LANES), jnp.float32)
        here[:, 0 : named.shape[1]] = by_expert
        for d in range(1, n_expert):
            remote(here, here, {"expert": (me + d) % n_expert}, parts, "shares")

    def history(d):
        start = pl.multiple_of(partner(my_dp, d) * cols, LANES)
        where = {"dp": partner(my_dp, d)}
        remote(prev.at[:, pl.ds(start, cols)], hx.at[d], where, hists, "hist")
        remote(prev.at[:, 0:HESS_COLS], hh.at[d], where, heads, "head")

    def activate(s):
        if s == 0:
            arrived(share_all.at[1:n_expert], "shares")
        table = share_all[...]
        expert = lax.broadcasted_iota(jnp.int32, table.shape, 1)
        table = jnp.sum(jnp.where(expert == me, table, 0.0), axis=1)
        table = jnp.concatenate(
            [table, jnp.zeros((LANES - n_expert, LANES), jnp.float32)], axis=0
        ).T
        for at in range(n_expert):
            kind, chip = at // chips, at % chips
            span = slice(at * rows, (at + 1) * rows)
            own_share = table[s * rows : (s + 1) * rows, at : at + 1]
            g = g_acc[span, :]
            hid[s, (kind + core + 1) % 2, chip * rows : (chip + 1) * rows, :] = (
                g / (1.0 + jnp.exp(-g)) * u_acc[span, :] * own_share
            ).astype(jnp.bfloat16)

    def down(s, i):
        j = s * n_dp + i
        if (s, i) == (0, 0):
            loaded(wd, down_sem)
        h = hid[s].reshape(n_expert * rows, hidden_w)
        for n in range(0, cols, tile):
            at = slice(n, n + tile)
            out = jnp.dot(h, wd[i, :, at], preferred_element_type=jnp.float32)
            out = out.reshape(2, chips, rows, tile)
            sb0[j, :, :, at] = out[0].astype(jnp.bfloat16)
            mine[j, :, :, at] = out[1]
        remote(sb0.at[j], rb0.at[j], to_peer, peers, (s, i, 0))

    def both(j, chip, part):
        return mine[j, chip, part, :] + rb0[j, chip, part, :].astype(jnp.float32)

    def first(s, i):
        j = s * n_dp + i
        arrived(rb0.at[j], (s, i, 0))
        for k in range(2):
            sb1[j, 0, k] = both(j, k * 2 + 1 - xx, low).astype(jnp.bfloat16)
        remote(sb1.at[j, 0], rb1.at[j, 0], to_x, firsts, (s, i, 1))
        for k in range(2):
            sb1[j, 1, k] = both(j, (1 - yy) * 2 + k, high).astype(jnp.bfloat16)
        remote(sb1.at[j, 1], rb1.at[j, 1], to_y, firsts, (s, i, 2))

    def second(s, i):
        j = s * n_dp + i
        arrived(rb1.at[j, 0], (s, i, 1))
        out = both(j, (1 - yy) * 2 + xx, low) + rb1[j, 0, 1 - yy].astype(jnp.float32)
        sb2[j, 0] = out.astype(jnp.bfloat16)
        remote(sb2.at[j, 0], rb2.at[j, 0], to_y, seconds, (s, i, 3))
        arrived(rb1.at[j, 1], (s, i, 2))
        out = both(j, yy * 2 + 1 - xx, high) + rb1[j, 1, 1 - xx].astype(jnp.float32)
        sb2[j, 1] = out.astype(jnp.bfloat16)
        remote(sb2.at[j, 1], rb2.at[j, 1], to_x, seconds, (s, i, 3))

    def third(s, i):
        j = s * n_dp + i
        d = turns[i]
        chip = me // 2
        arrived(rb2.at[j], (s, i, 3))
        top = both(j, chip, low) + rb1[j, 0, yy].astype(jnp.float32)
        top = top + rb2[j, 0].astype(jnp.float32)
        end = both(j, chip, high) + rb1[j, 1, xx].astype(jnp.float32)
        end = end + rb2[j, 1].astype(jnp.float32)
        if d:
            sb3[s, d - 1, low, :] = top.astype(jnp.bfloat16)
            sb3[s, d - 1, high, :] = end.astype(jnp.bfloat16)
            where = {"dp": partner(my_dp, d)}
            remote(sb3.at[s, d - 1], rb3.at[s, d - 1], where, thirds, (s, "over"))
        else:
            arrived(rb3.at[s], (s, "over"))
            for other in range(1, n_dp):
                top = top + rb3[s, other - 1, low, :].astype(jnp.float32)
                end = end + rb3[s, other - 1, high, :].astype(jnp.float32)
            mixed_ref[s * rows : s * rows + half, :] = top.astype(jnp.bfloat16)
            mixed_ref[s * rows + half : (s + 1) * rows, :] = end.astype(jnp.bfloat16)

    def gram():
        loaded(hx.at[0], hist_sem)
        loaded(hh.at[0], head_sem)
        arrived(hx.at[1:n_dp], "hist")
        arrived(hh.at[1:n_dp], "head")
        scale = 2.0 / (n_dp * hx.shape[1])

        @pl.loop(0, cols // tile)
        def _(n):
            at = pl.multiple_of(n * tile, tile)
            left = hx[:, :, pl.ds(at, tile)].reshape(n_dp * hx.shape[1], tile)
            right = hh[...].reshape(n_dp * hx.shape[1], HESS_COLS)
            product = lax.dot_general(
                left, right, (((0,), (0,)), ((), ())), preferred_element_type=jnp.float32
            )
            hess_ref[pl.ds(at, tile), :] = product * scale

    own(0, 0)
    own(0, 1)
    send_shares()
    history(2)
    own(0, 2)
    relay(0, 0)
    own(0, 3)
    own(1, 0)
    relay(0, 1)
    own(1, 1)
    corner(0, 0)
    relay(0, 2)
    own(1, 2)
    own(1, 3)
    widen(0, 0)
    corner(0, 1)
    widen(0, 1)
    relay(1, 0)
    corner(0, 2)
    arrive(0)
    widen(0, 2)
    relay(1, 1)
    widen(0, 3)
    activate(0)
    down(0, 0)
    corner(1, 0)
    history(1)
    history(3)
    relay(1, 2)
    down(0, 1)
    first(0, 0)
    corner(1, 1)
    down(0, 2)
    first(0, 1)
    corner(1, 2)
    widen(1, 0)
    first(0, 2)
    widen(1, 1)
    second(0, 0)
    widen(1, 2)
    arrive(1)
    second(0, 1)
    widen(1, 3)
    activate(1)
    down(1, 0)
    down(1, 1)
    first(1, 0)
    second(0, 2)
    third(0, 0)
    down(1, 2)
    first(1, 1)
    third(0, 1)
    down(0, 3)
    third(0, 2)
    down(1, 3)
    second(1, 0)
    first(1, 2)
    second(1, 1)
    first(0, 3)
    gram()
    third(1, 0)
    second(1, 2)
    first(1, 3)
    third(1, 1)
    second(0, 3)
    third(1, 2)
    second(1, 3)
    third(0, 3)
    third(1, 3)
    departed(mine.at[0 : mine.shape[0] - 1], gathers)
    departed(sb0, peers)
    departed(sb1, firsts)
    departed(sb2, seconds)
    departed(sb3, thirds)
    departed(hx.at[1:n_dp], hists)
    departed(hh.at[1:n_dp], heads)
    departed(share_all.at[1:n_expert], parts)


def store_kernel(mixed, hess, mixed_out, hess_out, sem):
    copies = [
        pltpu.make_async_copy(hess, hess_out, sem.at[0]),
        pltpu.make_async_copy(mixed, mixed_out, sem.at[1]),
    ]
    for copy in copies:
        copy.start()
    for copy in copies:
        copy.wait()


def everyone(tokens, routes, route_weight, w_gate, w_up, w_down, prev_inputs):
    total_rows, width = tokens.shape
    n_expert = lax.axis_size("expert")
    n_dp = lax.axis_size("dp")
    hidden_w = w_gate.shape[2]
    prev = prev_inputs.reshape(prev_inputs.shape[2], width)
    cols = width // n_dp
    chunks = 4
    depth = width // chunks
    chips = n_expert // 2
    rows = total_rows // SUBS
    half = rows // 2
    steps = SUBS * n_dp
    bf16, f32 = jnp.bfloat16, jnp.float32
    arrivals = SUBS * (4 * chunks - 2) + SUBS * (4 * n_dp + 1) + 3
    vmem = pl.BlockSpec(memory_space=pltpu.VMEM)
    hbm = pl.BlockSpec(memory_space=pl.ANY)
    mixed, hess = pl.pallas_call(
        functools.partial(dense_kernel, n_dp, n_expert),
        out_shape=(
            pltpu.VMEM((total_rows, cols), bf16),
            pltpu.VMEM((cols, HESS_COLS), f32),
        ),
        in_specs=[hbm] * 7,
        out_specs=(vmem, vmem),
        scratch_shapes=[
            pltpu.VMEM((SUBS, chunks, 2, chips, rows, depth), bf16),
            pltpu.VMEM((n_expert, n_expert, LANES), f32),
            pltpu.VMEM((chunks, depth, hidden_w), bf16),
            pltpu.VMEM((chunks, depth, hidden_w), bf16),
            pltpu.VMEM((n_dp, hidden_w, cols), bf16),
            pltpu.VMEM((n_expert * rows, hidden_w), f32),
            pltpu.VMEM((n_expert * rows, hidden_w), f32),
            pltpu.VMEM((SUBS, 2, chips * rows, hidden_w), bf16),
            pltpu.VMEM((steps, chips, rows, cols), f32),
            pltpu.VMEM((steps, chips, rows, cols), bf16),
            pltpu.VMEM((steps, chips, rows, cols), bf16),
            pltpu.VMEM((steps, 2, 2, half, cols), bf16),
            pltpu.VMEM((steps, 2, 2, half, cols), bf16),
            pltpu.VMEM((steps, 2, half, cols), bf16),
            pltpu.VMEM((steps, 2, half, cols), bf16),
            pltpu.VMEM((SUBS, n_dp - 1, rows, cols), bf16),
            pltpu.VMEM((SUBS, n_dp - 1, rows, cols), bf16),
            pltpu.VMEM((n_dp, prev.shape[0], cols), bf16),
            pltpu.VMEM((n_dp, prev.shape[0], HESS_COLS), bf16),
            pltpu.VMEM((routes.shape[1], total_rows), jnp.int32),
            pltpu.VMEM((routes.shape[1], total_rows), jnp.int32),
            pltpu.SemaphoreType.DMA((8,)),
            pltpu.SemaphoreType.DMA((8,)),
            pltpu.SemaphoreType.DMA((arrivals,)),
        ],
        compiler_params=pltpu.CompilerParams(
            collective_id=0, has_side_effects=True, vmem_limit_bytes=58000000
        ),
        name="dense_layer",
    )(tokens, routes.T, route_weight.T, w_gate[0], w_up[0], w_down[0], prev)
    mixed, hess = pl.pallas_call(
        store_kernel,
        out_shape=(
            jax.ShapeDtypeStruct(mixed.shape, bf16),
            jax.ShapeDtypeStruct(hess.shape, f32),
        ),
        in_specs=[vmem] * 2,
        out_specs=(hbm, hbm),
        scratch_shapes=[pltpu.SemaphoreType.DMA((2,))],
        compiler_params=pltpu.CompilerParams(vmem_limit_bytes=4194304),
        name="store_outputs",
    )(mixed, hess)
    return mixed, hess.reshape(cols, 1, HESS_COLS)


def shards(tokens, routes, route_weight, w_gate, w_up, w_down, prev_inputs):
    n_expert = lax.axis_size("expert")
    n_dp = lax.axis_size("dp")
    if w_gate.shape[0] == 1 and routes.shape[1] == n_expert == 2 * 2 * 2 and n_dp == 2 * 2:
        return everyone(tokens, routes, route_weight, w_gate, w_up, w_down, prev_inputs)
    hessian = gram_window(prev_inputs, n_dp, tokens.shape[1])
    return slotted(tokens, routes, route_weight, w_gate, w_up, w_down), hessian


def solution(mesh):
    placed = (
        P("expert", None),
        P("expert", None),
        P("expert", None),
        P("expert", None, "dp"),
        P("expert", None, "dp"),
        P("expert", "dp", None),
        P("dp", "expert", None, None),
    )
    return jax.shard_map(
        shards,
        mesh=mesh,
        in_specs=placed,
        out_specs=(P("expert", "dp"), P("dp", "expert", None)),
        check_vma=False,
    )
```

```python
import functools

import jax
import jax.numpy as jnp
from jax import lax
from jax.experimental import pallas as pl
from jax.experimental.pallas import tpu as pltpu
from jax.sharding import PartitionSpec as P

HESS_COLS = 128


def route_slots(flat_ids, experts_all):
    onehot = (flat_ids[:, None] == jnp.arange(experts_all, dtype=jnp.int32)[None, :]).astype(
        jnp.int32
    )
    earlier = jnp.cumsum(onehot, axis=0) - onehot
    return jnp.sum(earlier * onehot, axis=1)


def combine_rows(back, places, shares, tok_dev, top):
    columns = back.shape[-1]
    rows = back.reshape(-1, columns)[places]
    weighted = rows.astype(jnp.float32) * shares.reshape(-1, 1)
    return jnp.sum(weighted.reshape(tok_dev, top, columns), axis=1)


def route_shares(route_weight):
    weight_counts = route_weight.astype(jnp.float32)
    return 2.5 * weight_counts / jnp.sum(weight_counts, axis=1, keepdims=True)


def gram_window(prev_inputs, n_dp, width):
    history = prev_inputs.reshape(prev_inputs.shape[1], prev_inputs.shape[2], width)
    head_cols = history[:, :, :HESS_COLS]
    gram_scale = 2.0 / (n_dp * history.shape[1])
    return lax.psum_scatter(
        (
            jnp.einsum("jrd,jrh->djh", history, head_cols, preferred_element_type=jnp.float32)
            * gram_scale
        ).astype(jnp.bfloat16),
        "dp",
        scatter_dimension=0,
        tiled=True,
    ).astype(jnp.float32)


def slotted(tokens, routes, route_weight, w_gate, w_up, w_down):
    tok_dev, top = routes.shape
    exp_dev = w_gate.shape[0]
    width = tokens.shape[1]
    n_expert = lax.axis_size("expert")
    experts_all = exp_dev * n_expert
    capacity = min(tok_dev, tok_dev * top * 5 // (4 * experts_all))
    flat_ids = routes.reshape(-1)
    slots = route_slots(flat_ids, experts_all)
    places = flat_ids * capacity + slots
    shares = route_shares(route_weight)
    picks = jnp.arange(experts_all * capacity, dtype=jnp.int32)[:, None] == places[None, :]
    placing = jnp.any(picks.reshape(experts_all * capacity, tok_dev, top), axis=2).astype(
        jnp.bfloat16
    )
    outgoing = jnp.dot(placing, tokens, preferred_element_type=jnp.float32).astype(jnp.bfloat16)
    outgoing = outgoing.reshape(experts_all, capacity, width)
    arrived = lax.all_to_all(outgoing, "expert", split_axis=0, concat_axis=0, tiled=True)
    arrived = arrived.reshape(n_expert, exp_dev, capacity, width)
    gate = jnp.einsum("sjcd,jdf->sjcf", arrived, w_gate, preferred_element_type=jnp.float32)
    up = jnp.einsum("sjcd,jdf->sjcf", arrived, w_up, preferred_element_type=jnp.float32)
    hidden = (jax.nn.silu(gate) * up).astype(jnp.bfloat16)
    partial_out = jnp.einsum("sjcf,jfd->sjcd", hidden, w_down, preferred_element_type=jnp.float32)
    partial_out = partial_out.astype(jnp.bfloat16)
    back = lax.all_to_all(
        partial_out.reshape(experts_all, capacity, width),
        "expert",
        split_axis=0,
        concat_axis=0,
        tiled=True,
    )
    own_sum = combine_rows(back, places, shares, tok_dev, top)
    return lax.psum_scatter(own_sum.astype(jnp.bfloat16), "dp", scatter_dimension=1, tiled=True)

LANES = 128
SUBS = 2
MESH = pl.DeviceIdType.MESH


def flip(index, bit):
    return index + bit - 2 * bit * ((index // bit) % 2)


def partner(index, mask):
    bit = 1
    while bit <= mask:
        if mask & bit:
            index = flip(index, bit)
        bit *= 2
    return index


def dense_kernel(
    n_dp,
    n_expert,
    tokens,
    routes,
    route_weight,
    w_gate,
    w_up,
    w_down,
    prev,
    mixed_ref,
    hess_ref,
    xall,
    share_all,
    wg,
    wu,
    wd,
    g_acc,
    u_acc,
    hid,
    mine,
    sb0,
    rb0,
    sb1,
    rb1,
    sb2,
    rb2,
    sb3,
    rb3,
    hx,
    hh,
    ids,
    counts,
    lsem,
    send_sem,
    recv_sem,
    round_sem,
):
    me = lax.axis_index("expert")
    my_dp = lax.axis_index("dp")
    core, xx, yy = me % 2, (me // 2) % 2, (me // 4) % 2
    peer, ex, ey = flip(me, 1), flip(me, 2), flip(me, 4)
    ed = flip(ex, 4)
    subs, chunks, depth = xall.shape[0], xall.shape[1], xall.shape[-1]
    rows = xall.shape[4]
    half = rows // 2
    chips = n_expert // 2
    cols = rb3.shape[-1]
    hidden_w = wg.shape[-1]
    tokens_sem, gate_sem, up_sem, down_sem, hist_sem, head_sem, ids_sem, counts_sem = range(8)
    gathers, peers, firsts, seconds, thirds, hists, heads, parts = range(8)
    lanes = {}

    def local(src, dst, sem):
        pltpu.make_async_copy(src, dst, lsem.at[sem]).start()

    def loaded(ref, sem):
        pltpu.make_async_copy(ref, ref, lsem.at[sem]).wait()

    def describe(src, dst, where, group, key):
        return pltpu.make_async_remote_copy(
            src_ref=src,
            dst_ref=dst,
            send_sem=send_sem.at[group],
            recv_sem=recv_sem.at[lanes.setdefault(key, len(lanes))],
            device_id=where,
            device_id_type=MESH,
        )

    def remote(src, dst, where, group, key):
        describe(src, dst, where, group, key).start()

    def arrived(ref, key):
        describe(ref, ref, to_peer, 0, key).wait_recv()

    def departed(ref, group):
        describe(ref, ref, to_peer, group, (0, 0, "x")).wait_send()

    side = my_dp % 2
    last = chunks - 1

    def piece(c):
        return pl.ds(pl.multiple_of((side * last + c * (1 - 2 * side)) * depth, LANES), depth)

    for s in range(subs):
        for c in range(chunks):
            local(
                tokens.at[s * rows : (s + 1) * rows, piece(c)],
                xall.at[s, c, core, me // 2],
                tokens_sem,
            )
    local(routes, ids, ids_sem)
    local(route_weight, counts, counts_sem)
    for c in range(chunks):
        local(w_gate.at[piece(c), :], wg.at[c], gate_sem)
        local(w_up.at[piece(c), :], wu.at[c], up_sem)
    pair = my_dp // 2
    inner = (my_dp + pair) % 2
    turns = [
        ((n_dp - 1) * (1 - pair), 3 - inner),
        (n_dp // 2 - pair, 2 + inner),
        (flip(my_dp, 1), 1),
        (my_dp, 0),
    ]
    for i, (owner, _) in enumerate(turns):
        start = pl.multiple_of(owner * cols, LANES)
        local(w_down.at[:, pl.ds(start, cols)], wd.at[i], down_sem)
    local(prev.at[:, pl.ds(pl.multiple_of(my_dp * cols, LANES), cols)], hx.at[0], hist_sem)
    local(prev.at[:, 0:HESS_COLS], hh.at[0], head_sem)

    to_peer, to_x, to_y = {"expert": peer}, {"expert": ex}, {"expert": ey}
    has_lower = (my_dp + n_dp - 1) // n_dp
    has_upper = (n_dp - 1 - my_dp + n_dp - 1) // n_dp

    def greet(sem):
        for where in (to_peer, to_x, to_y):
            pl.semaphore_signal(sem, inc=1, device_id=where, device_id_type=MESH)
        for exists, where in ((has_lower, my_dp - 1), (has_upper, my_dp + 1)):

            @pl.when(exists == 1)
            def _():
                pl.semaphore_signal(sem, inc=1, device_id={"dp": where}, device_id_type=MESH)

    def met(sem):
        pl.semaphore_wait(sem, 3 + has_lower + has_upper)

    def rounds(n):
        greet(round_sem.at[n])
        met(round_sem.at[n])

    barrier = pltpu.get_barrier_semaphore()
    greet(barrier)
    met(barrier)

    to_z = {"dp": flip(my_dp, 1)}

    def block(s, c, who):
        return xall.at[s, c, who % 2, who // 2]

    def own(s, c):
        if (s, c) == (0, 0):
            loaded(tokens, tokens_sem)
        here = block(s, c, me)
        if c < last:
            remote(here, here, to_x, gathers, (s, c, "x"))
            remote(here, here, to_y, gathers, (s, c, "y"))
        remote(here, here, to_peer, gathers, (s, c, "p"))

    def share_block(s, c, who):
        remote(block(s, c, who), block(s, c, who), to_peer, gathers, (s, c, "p"))

    def across(s, who):
        remote(block(s, 0, who), block(s, last, who), to_z, gathers, (s, "z"))

    low, high = slice(0, half), slice(half, rows)

    def relay(s, c):
        for name, who, forth, part in (("x", ex, to_y, low), ("y", ey, to_x, high)):
            here = block(s, c, who)
            arrived(here, (s, c, name))
            remote(here.at[part], here.at[part], forth, gathers, (s, c, "d"))
            if c == 0:
                across(s, who)
            share_block(s, c, who)

    def corner(s, c):
        arrived(block(s, c, ed), (s, c, "d"))
        if c == 0:
            across(s, ed)
        share_block(s, c, ed)

    def arrive(s):
        arrived(xall.at[s, last, core, 1:chips], (s, "z"))
        for who in (ex, ey, ed):
            share_block(s, last, who)

    tile = 2 * LANES

    def widen(s, c):
        arrived(xall.at[s, c, 1 - core], (s, c, "p"))
        if (s, c) == (0, 0):
            loaded(wg, gate_sem)
            loaded(wu, up_sem)
        x = xall[s, c].reshape(n_expert * rows, depth)
        for n in range(0, hidden_w, tile):
            at = slice(n, n + tile)
            g = jnp.dot(x, wg[c, :, at], preferred_element_type=jnp.float32)
            u = jnp.dot(x, wu[c, :, at], preferred_element_type=jnp.float32)
            if c == 0:
                g_acc[:, at] = g
                u_acc[:, at] = u
            else:
                g_acc[:, at] += g
                u_acc[:, at] += u

    def send_shares():
        loaded(ids, ids_sem)
        loaded(counts, counts_sem)
        weight = counts[...].astype(jnp.float32)
        part = 2.5 * weight / jnp.sum(weight, axis=0, keepdims=True)
        named = ids[...]
        expert = lax.broadcasted_iota(jnp.int32, (n_expert, named.shape[1]), 0)
        by_expert = jnp.zeros(expert.shape, jnp.float32)
        for k in range(named.shape[0]):
            by_expert += jnp.where(named[k : k + 1, :] == expert, part[k : k + 1, :], 0.0)
        here = share_all.at[core * chips + me // 2]
        here[...] = jnp.zeros((n_expert, LANES), jnp.float32)
        here[:, 0 : named.shape[1]] = by_expert
        for d in range(1, n_expert):
            remote(here, here, {"expert": (me + d) % n_expert}, parts, "shares")

    def history(d, first_half=True, second_half=True):
        count = hx.shape[1]
        take = slice(0 if first_half else count // 2, count if second_half else count // 2)
        start = pl.multiple_of(partner(my_dp, d) * cols, LANES)
        where = {"dp": partner(my_dp, d)}
        remote(prev.at[take, pl.ds(start, cols)], hx.at[d, take], where, hists, "hist")
        remote(prev.at[take, 0:HESS_COLS], hh.at[d, take], where, heads, "head")

    def activate(s):
        if s == 0:
            arrived(share_all.at[1:n_expert], "shares")
        table = share_all[...]
        expert = lax.broadcasted_iota(jnp.int32, table.shape, 1)
        table = jnp.sum(jnp.where(expert == me, table, 0.0), axis=1)
        table = jnp.concatenate(
            [table, jnp.zeros((LANES - n_expert, LANES), jnp.float32)], axis=0
        ).T
        for at in range(n_expert):
            kind, chip = at // chips, at % chips
            span = slice(at * rows, (at + 1) * rows)
            own_share = table[s * rows : (s + 1) * rows, at : at + 1]
            g = g_acc[span, :]
            hid[s, (kind + core + 1) % 2, chip * rows : (chip + 1) * rows, :] = (
                g / (1.0 + jnp.exp(-g)) * u_acc[span, :] * own_share
            ).astype(jnp.bfloat16)

    def down(s, i):
        j = s * n_dp + i
        if (s, i) == (0, 0):
            loaded(wd, down_sem)
        h = hid[s].reshape(n_expert * rows, hidden_w)
        for n in range(0, cols, tile):
            at = slice(n, n + tile)
            out = jnp.dot(h, wd[i, :, at], preferred_element_type=jnp.float32)
            out = out.reshape(2, chips, rows, tile)
            sb0[j, :, :, at] = out[0].astype(jnp.bfloat16)
            mine[j, :, :, at] = out[1]
        remote(sb0.at[j], rb0.at[j], to_peer, peers, (s, i, 0))

    def both(j, chip, part):
        return mine[j, chip, part, :] + rb0[j, chip, part, :].astype(jnp.float32)

    def first(s, i):
        j = s * n_dp + i
        arrived(rb0.at[j], (s, i, 0))
        for k in range(2):
            sb1[j, 0, k] = both(j, k * 2 + 1 - xx, low).astype(jnp.bfloat16)
        remote(sb1.at[j, 0], rb1.at[j, 0], to_x, firsts, (s, i, 1))
        for k in range(2):
            sb1[j, 1, k] = both(j, (1 - yy) * 2 + k, high).astype(jnp.bfloat16)
        remote(sb1.at[j, 1], rb1.at[j, 1], to_y, firsts, (s, i, 2))

    def second(s, i):
        j = s * n_dp + i
        arrived(rb1.at[j, 0], (s, i, 1))
        out = both(j, (1 - yy) * 2 + xx, low) + rb1[j, 0, 1 - yy].astype(jnp.float32)
        sb2[j, 0] = out.astype(jnp.bfloat16)
        remote(sb2.at[j, 0], rb2.at[j, 0], to_y, seconds, (s, i, 3))
        arrived(rb1.at[j, 1], (s, i, 2))
        out = both(j, yy * 2 + 1 - xx, high) + rb1[j, 1, 1 - xx].astype(jnp.float32)
        sb2[j, 1] = out.astype(jnp.bfloat16)
        remote(sb2.at[j, 1], rb2.at[j, 1], to_x, seconds, (s, i, 3))

    def third(s, i):
        j = s * n_dp + i
        owner, mask = turns[i]
        chip = me // 2
        arrived(rb2.at[j], (s, i, 3))
        top = both(j, chip, low) + rb1[j, 0, yy].astype(jnp.float32)
        top = top + rb2[j, 0].astype(jnp.float32)
        end = both(j, chip, high) + rb1[j, 1, xx].astype(jnp.float32)
        end = end + rb2[j, 1].astype(jnp.float32)
        if i < n_dp - 1:
            sb3[s, i, low, :] = top.astype(jnp.bfloat16)
            sb3[s, i, high, :] = end.astype(jnp.bfloat16)
            remote(sb3.at[s, i], rb3.at[s, mask - 1], {"dp": owner}, thirds, (s, "over"))
        else:
            arrived(rb3.at[s], (s, "over"))
            for other in range(1, n_dp):
                top = top + rb3[s, other - 1, low, :].astype(jnp.float32)
                end = end + rb3[s, other - 1, high, :].astype(jnp.float32)
            mixed_ref[s * rows : s * rows + half, :] = top.astype(jnp.bfloat16)
            mixed_ref[s * rows + half : (s + 1) * rows, :] = end.astype(jnp.bfloat16)

    def gram():
        loaded(hx.at[0], hist_sem)
        loaded(hh.at[0], head_sem)
        arrived(hx.at[1:n_dp], "hist")
        arrived(hh.at[1:n_dp], "head")
        scale = 2.0 / (n_dp * hx.shape[1])

        @pl.loop(0, cols // tile)
        def _(n):
            at = pl.multiple_of(n * tile, tile)
            left = hx[:, :, pl.ds(at, tile)].reshape(n_dp * hx.shape[1], tile)
            right = hh[...].reshape(n_dp * hx.shape[1], HESS_COLS)
            product = lax.dot_general(
                left, right, (((0,), (0,)), ((), ())), preferred_element_type=jnp.float32
            )
            hess_ref[pl.ds(at, tile), :] = product * scale

    own(0, 0)
    own(0, 1)
    own(0, 2)
    rounds(0)
    history(2)
    rounds(1)
    send_shares()
    relay(0, 0)
    own(0, 3)
    relay(0, 1)
    own(1, 0)
    relay(0, 2)
    own(1, 1)
    corner(0, 0)
    corner(0, 1)
    widen(0, 0)
    widen(0, 1)
    relay(1, 0)
    own(1, 2)
    own(1, 3)
    corner(0, 2)
    arrive(0)
    widen(0, 2)
    relay(1, 1)
    widen(0, 3)
    corner(1, 0)
    activate(0)
    down(0, 0)
    down(0, 1)
    relay(1, 2)
    first(0, 0)
    history(3)
    history(1)
    down(0, 2)
    first(0, 1)
    corner(1, 1)
    widen(1, 0)
    first(0, 2)
    widen(1, 1)
    corner(1, 2)
    arrive(1)
    widen(1, 2)
    widen(1, 3)
    second(0, 0)
    activate(1)
    down(1, 0)
    down(1, 1)
    second(0, 1)
    first(1, 0)
    down(1, 2)
    second(0, 2)
    first(1, 1)
    third(0, 0)
    down(1, 3)
    third(0, 1)
    down(0, 3)
    second(1, 0)
    first(1, 2)
    third(0, 2)
    second(1, 1)
    third(1, 0)
    first(0, 3)
    gram()
    second(1, 2)
    third(1, 1)
    first(1, 3)
    second(0, 3)
    third(1, 2)
    second(1, 3)
    third(0, 3)
    third(1, 3)
    departed(mine.at[0 : mine.shape[0] - 1], gathers)
    departed(sb0, peers)
    departed(sb1, firsts)
    departed(sb2, seconds)
    departed(sb3, thirds)
    departed(hx.at[1:n_dp], hists)
    departed(hh.at[1:n_dp], heads)
    departed(share_all.at[1:n_expert], parts)


def store_kernel(mixed, hess, mixed_out, hess_out, sem):
    copies = [
        pltpu.make_async_copy(hess, hess_out, sem.at[0]),
        pltpu.make_async_copy(mixed, mixed_out, sem.at[1]),
    ]
    for copy in copies:
        copy.start()
    for copy in copies:
        copy.wait()


def everyone(tokens, routes, route_weight, w_gate, w_up, w_down, prev_inputs):
    total_rows, width = tokens.shape
    n_expert = lax.axis_size("expert")
    n_dp = lax.axis_size("dp")
    hidden_w = w_gate.shape[2]
    prev = prev_inputs.reshape(prev_inputs.shape[2], width)
    cols = width // n_dp
    chunks = 4
    depth = width // chunks
    chips = n_expert // 2
    rows = total_rows // SUBS
    half = rows // 2
    steps = SUBS * n_dp
    bf16, f32 = jnp.bfloat16, jnp.float32
    arrivals = SUBS * (4 * chunks - 2) + SUBS * (4 * n_dp + 1) + 3
    vmem = pl.BlockSpec(memory_space=pltpu.VMEM)
    hbm = pl.BlockSpec(memory_space=pl.ANY)
    mixed, hess = pl.pallas_call(
        functools.partial(dense_kernel, n_dp, n_expert),
        out_shape=(
            pltpu.VMEM((total_rows, cols), bf16),
            pltpu.VMEM((cols, HESS_COLS), f32),
        ),
        in_specs=[hbm] * 7,
        out_specs=(vmem, vmem),
        scratch_shapes=[
            pltpu.VMEM((SUBS, chunks, 2, chips, rows, depth), bf16),
            pltpu.VMEM((n_expert, n_expert, LANES), f32),
            pltpu.VMEM((chunks, depth, hidden_w), bf16),
            pltpu.VMEM((chunks, depth, hidden_w), bf16),
            pltpu.VMEM((n_dp, hidden_w, cols), bf16),
            pltpu.VMEM((n_expert * rows, hidden_w), f32),
            pltpu.VMEM((n_expert * rows, hidden_w), f32),
            pltpu.VMEM((SUBS, 2, chips * rows, hidden_w), bf16),
            pltpu.VMEM((steps, chips, rows, cols), f32),
            pltpu.VMEM((steps, chips, rows, cols), bf16),
            pltpu.VMEM((steps, chips, rows, cols), bf16),
            pltpu.VMEM((steps, 2, 2, half, cols), bf16),
            pltpu.VMEM((steps, 2, 2, half, cols), bf16),
            pltpu.VMEM((steps, 2, half, cols), bf16),
            pltpu.VMEM((steps, 2, half, cols), bf16),
            pltpu.VMEM((SUBS, n_dp - 1, rows, cols), bf16),
            pltpu.VMEM((SUBS, n_dp - 1, rows, cols), bf16),
            pltpu.VMEM((n_dp, prev.shape[0], cols), bf16),
            pltpu.VMEM((n_dp, prev.shape[0], HESS_COLS), bf16),
            pltpu.VMEM((routes.shape[1], total_rows), jnp.int32),
            pltpu.VMEM((routes.shape[1], total_rows), jnp.int32),
            pltpu.SemaphoreType.DMA((8,)),
            pltpu.SemaphoreType.DMA((8,)),
            pltpu.SemaphoreType.DMA((arrivals,)),
            pltpu.SemaphoreType.REGULAR((2,)),
        ],
        compiler_params=pltpu.CompilerParams(
            collective_id=0, has_side_effects=True, vmem_limit_bytes=58000000
        ),
        name="dense_layer",
    )(tokens, routes.T, route_weight.T, w_gate[0], w_up[0], w_down[0], prev)
    mixed, hess = pl.pallas_call(
        store_kernel,
        out_shape=(
            jax.ShapeDtypeStruct(mixed.shape, bf16),
            jax.ShapeDtypeStruct(hess.shape, f32),
        ),
        in_specs=[vmem] * 2,
        out_specs=(hbm, hbm),
        scratch_shapes=[pltpu.SemaphoreType.DMA((2,))],
        compiler_params=pltpu.CompilerParams(vmem_limit_bytes=4194304),
        name="store_outputs",
    )(mixed, hess)
    return mixed, hess.reshape(cols, 1, HESS_COLS)


def shards(tokens, routes, route_weight, w_gate, w_up, w_down, prev_inputs):
    n_expert = lax.axis_size("expert")
    n_dp = lax.axis_size("dp")
    if w_gate.shape[0] == 1 and routes.shape[1] == n_expert == 2 * 2 * 2 and n_dp == 2 * 2:
        return everyone(tokens, routes, route_weight, w_gate, w_up, w_down, prev_inputs)
    hessian = gram_window(prev_inputs, n_dp, tokens.shape[1])
    return slotted(tokens, routes, route_weight, w_gate, w_up, w_down), hessian


def solution(mesh):
    placed = (
        P("expert", None),
        P("expert", None),
        P("expert", None),
        P("expert", None, "dp"),
        P("expert", None, "dp"),
        P("expert", "dp", None),
        P("dp", "expert", None, None),
    )
    return jax.shard_map(
        shards,
        mesh=mesh,
        in_specs=placed,
        out_specs=(P("expert", "dp"), P("dp", "expert", None)),
        check_vma=False,
    )
```

```python
import functools

import jax
import jax.numpy as jnp
from jax import lax
from jax.experimental import pallas as pl
from jax.experimental.pallas import tpu as pltpu
from jax.sharding import PartitionSpec as P

HESS_COLS = 128


def route_slots(flat_ids, experts_all):
    onehot = (flat_ids[:, None] == jnp.arange(experts_all, dtype=jnp.int32)[None, :]).astype(
        jnp.int32
    )
    earlier = jnp.cumsum(onehot, axis=0) - onehot
    return jnp.sum(earlier * onehot, axis=1)


def combine_rows(back, places, shares, tok_dev, top):
    columns = back.shape[-1]
    rows = back.reshape(-1, columns)[places]
    weighted = rows.astype(jnp.float32) * shares.reshape(-1, 1)
    return jnp.sum(weighted.reshape(tok_dev, top, columns), axis=1)


def route_shares(route_weight):
    weight_counts = route_weight.astype(jnp.float32)
    return 2.5 * weight_counts / jnp.sum(weight_counts, axis=1, keepdims=True)


def gram_window(prev_inputs, n_dp, width):
    history = prev_inputs.reshape(prev_inputs.shape[1], prev_inputs.shape[2], width)
    head_cols = history[:, :, :HESS_COLS]
    gram_scale = 2.0 / (n_dp * history.shape[1])
    return lax.psum_scatter(
        (
            jnp.einsum("jrd,jrh->djh", history, head_cols, preferred_element_type=jnp.float32)
            * gram_scale
        ).astype(jnp.bfloat16),
        "dp",
        scatter_dimension=0,
        tiled=True,
    ).astype(jnp.float32)


def slotted(tokens, routes, route_weight, w_gate, w_up, w_down):
    tok_dev, top = routes.shape
    exp_dev = w_gate.shape[0]
    width = tokens.shape[1]
    n_expert = lax.axis_size("expert")
    experts_all = exp_dev * n_expert
    capacity = min(tok_dev, tok_dev * top * 5 // (4 * experts_all))
    flat_ids = routes.reshape(-1)
    slots = route_slots(flat_ids, experts_all)
    places = flat_ids * capacity + slots
    shares = route_shares(route_weight)
    picks = jnp.arange(experts_all * capacity, dtype=jnp.int32)[:, None] == places[None, :]
    placing = jnp.any(picks.reshape(experts_all * capacity, tok_dev, top), axis=2).astype(
        jnp.bfloat16
    )
    outgoing = jnp.dot(placing, tokens, preferred_element_type=jnp.float32).astype(jnp.bfloat16)
    outgoing = outgoing.reshape(experts_all, capacity, width)
    arrived = lax.all_to_all(outgoing, "expert", split_axis=0, concat_axis=0, tiled=True)
    arrived = arrived.reshape(n_expert, exp_dev, capacity, width)
    gate = jnp.einsum("sjcd,jdf->sjcf", arrived, w_gate, preferred_element_type=jnp.float32)
    up = jnp.einsum("sjcd,jdf->sjcf", arrived, w_up, preferred_element_type=jnp.float32)
    hidden = (jax.nn.silu(gate) * up).astype(jnp.bfloat16)
    partial_out = jnp.einsum("sjcf,jfd->sjcd", hidden, w_down, preferred_element_type=jnp.float32)
    partial_out = partial_out.astype(jnp.bfloat16)
    back = lax.all_to_all(
        partial_out.reshape(experts_all, capacity, width),
        "expert",
        split_axis=0,
        concat_axis=0,
        tiled=True,
    )
    own_sum = combine_rows(back, places, shares, tok_dev, top)
    return lax.psum_scatter(own_sum.astype(jnp.bfloat16), "dp", scatter_dimension=1, tiled=True)

LANES = 128
SUBS = 2
MESH = pl.DeviceIdType.MESH


def flip(index, bit):
    return index + bit - 2 * bit * ((index // bit) % 2)


def partner(index, mask):
    bit = 1
    while bit <= mask:
        if mask & bit:
            index = flip(index, bit)
        bit *= 2
    return index


def dense_kernel(
    n_dp,
    n_expert,
    tokens,
    routes,
    route_weight,
    w_gate,
    w_up,
    w_down,
    prev,
    mixed_ref,
    hess_ref,
    xall,
    share_all,
    wg,
    wu,
    wd,
    g_acc,
    u_acc,
    hid,
    mine,
    sb0,
    rb0,
    sb1,
    rb1,
    sb2,
    rb2,
    sb3,
    rb3,
    hx,
    hh,
    ids,
    counts,
    lsem,
    send_sem,
    recv_sem,
    round_sem,
):
    me = lax.axis_index("expert")
    my_dp = lax.axis_index("dp")
    core, xx, yy = me % 2, (me // 2) % 2, (me // 4) % 2
    peer, ex, ey = flip(me, 1), flip(me, 2), flip(me, 4)
    ed = flip(ex, 4)
    subs, chunks, depth = xall.shape[0], xall.shape[1], xall.shape[-1]
    rows = xall.shape[4]
    half = rows // 2
    chips = n_expert // 2
    cols = rb3.shape[-1]
    hidden_w = wg.shape[-1]
    tokens_sem, gate_sem, up_sem, down_sem, hist_sem, head_sem, ids_sem, counts_sem = range(8)
    gathers, peers, firsts, seconds, thirds, hists, heads, parts = range(8)
    lanes = {}

    def local(src, dst, sem):
        pltpu.make_async_copy(src, dst, lsem.at[sem]).start()

    def loaded(ref, sem):
        pltpu.make_async_copy(ref, ref, lsem.at[sem]).wait()

    def describe(src, dst, where, group, key):
        return pltpu.make_async_remote_copy(
            src_ref=src,
            dst_ref=dst,
            send_sem=send_sem.at[group],
            recv_sem=recv_sem.at[lanes.setdefault(key, len(lanes))],
            device_id=where,
            device_id_type=MESH,
        )

    def remote(src, dst, where, group, key):
        describe(src, dst, where, group, key).start()

    def arrived(ref, key):
        describe(ref, ref, to_peer, 0, key).wait_recv()

    def departed(ref, group):
        describe(ref, ref, to_peer, group, (0, 0, "x")).wait_send()

    side = my_dp % 2
    last = chunks - 1

    def piece(c):
        return pl.ds(pl.multiple_of((side * last + c * (1 - 2 * side)) * depth, LANES), depth)

    for s in range(subs):
        for c in range(chunks):
            local(
                tokens.at[s * rows : (s + 1) * rows, piece(c)],
                xall.at[s, c, core, me // 2],
                tokens_sem,
            )
    local(routes, ids, ids_sem)
    local(route_weight, counts, counts_sem)
    for c in range(chunks):
        local(w_gate.at[piece(c), :], wg.at[c], gate_sem)
        local(w_up.at[piece(c), :], wu.at[c], up_sem)
    odd = my_dp % 2
    inner = (my_dp + my_dp // 2) % 2
    turns = [
        ((n_dp - 1) * (1 - odd), 3 - 2 * inner),
        (flip(my_dp, 2), 2),
        (1 + odd, 1 + 2 * inner),
        (my_dp, 0),
    ]
    for i, (owner, _) in enumerate(turns):
        start = pl.multiple_of(owner * cols, LANES)
        local(w_down.at[:, pl.ds(start, cols)], wd.at[i], down_sem)
    local(prev.at[:, pl.ds(pl.multiple_of(my_dp * cols, LANES), cols)], hx.at[0], hist_sem)
    local(prev.at[:, 0:HESS_COLS], hh.at[0], head_sem)

    to_peer, to_x, to_y = {"expert": peer}, {"expert": ex}, {"expert": ey}
    has_lower = (my_dp + n_dp - 1) // n_dp
    has_upper = (n_dp - 1 - my_dp + n_dp - 1) // n_dp

    def greet(sem):
        for where in (to_peer, to_x, to_y):
            pl.semaphore_signal(sem, inc=1, device_id=where, device_id_type=MESH)
        for exists, where in ((has_lower, my_dp - 1), (has_upper, my_dp + 1)):

            @pl.when(exists == 1)
            def _():
                pl.semaphore_signal(sem, inc=1, device_id={"dp": where}, device_id_type=MESH)

    def met(sem):
        pl.semaphore_wait(sem, 3 + has_lower + has_upper)

    def rounds(n):
        greet(round_sem.at[n])
        met(round_sem.at[n])

    barrier = pltpu.get_barrier_semaphore()
    greet(barrier)
    met(barrier)

    to_z = {"dp": flip(my_dp, 1)}

    def block(s, c, who):
        return xall.at[s, c, who % 2, who // 2]

    def own(s, c):
        if (s, c) == (0, 0):
            loaded(tokens, tokens_sem)
        here = block(s, c, me)
        if c < last:
            remote(here, here, to_x, gathers, (s, c, "x"))
            remote(here, here, to_y, gathers, (s, c, "y"))
        remote(here, here, to_peer, gathers, (s, c, "p"))

    def share_block(s, c, who):
        remote(block(s, c, who), block(s, c, who), to_peer, gathers, (s, c, "p"))

    def across(s, who):
        remote(block(s, 0, who), block(s, last, who), to_z, gathers, (s, "z"))

    low, high = slice(0, half), slice(half, rows)

    def relay(s, c):
        for name, who, forth, part in (("x", ex, to_y, low), ("y", ey, to_x, high)):
            here = block(s, c, who)
            arrived(here, (s, c, name))
            remote(here.at[part], here.at[part], forth, gathers, (s, c, "d"))
            if c == 0:
                across(s, who)
            share_block(s, c, who)

    def corner(s, c):
        arrived(block(s, c, ed), (s, c, "d"))
        if c == 0:
            across(s, ed)
        share_block(s, c, ed)

    def arrive(s):
        arrived(xall.at[s, last, core, 1:chips], (s, "z"))
        for who in (ex, ey, ed):
            share_block(s, last, who)

    tile = 2 * LANES

    def widen(s, c):
        arrived(xall.at[s, c, 1 - core], (s, c, "p"))
        if (s, c) == (0, 0):
            loaded(wg, gate_sem)
            loaded(wu, up_sem)
        x = xall[s, c].reshape(n_expert * rows, depth)
        for n in range(0, hidden_w, tile):
            at = slice(n, n + tile)
            g = jnp.dot(x, wg[c, :, at], preferred_element_type=jnp.float32)
            u = jnp.dot(x, wu[c, :, at], preferred_element_type=jnp.float32)
            if c == 0:
                g_acc[:, at] = g
                u_acc[:, at] = u
            else:
                g_acc[:, at] += g
                u_acc[:, at] += u

    def send_shares():
        loaded(ids, ids_sem)
        loaded(counts, counts_sem)
        weight = counts[...].astype(jnp.float32)
        part = 2.5 * weight / jnp.sum(weight, axis=0, keepdims=True)
        named = ids[...]
        expert = lax.broadcasted_iota(jnp.int32, (n_expert, named.shape[1]), 0)
        by_expert = jnp.zeros(expert.shape, jnp.float32)
        for k in range(named.shape[0]):
            by_expert += jnp.where(named[k : k + 1, :] == expert, part[k : k + 1, :], 0.0)
        here = share_all.at[core * chips + me // 2]
        here[...] = jnp.zeros((n_expert, LANES), jnp.float32)
        here[:, 0 : named.shape[1]] = by_expert
        for d in range(1, n_expert):
            remote(here, here, {"expert": (me + d) % n_expert}, parts, "shares")

    def history(d, first_half=True, second_half=True):
        count = hx.shape[1]
        take = slice(0 if first_half else count // 2, count if second_half else count // 2)
        start = pl.multiple_of(partner(my_dp, d) * cols, LANES)
        where = {"dp": partner(my_dp, d)}
        remote(prev.at[take, pl.ds(start, cols)], hx.at[d, take], where, hists, "hist")
        remote(prev.at[take, 0:HESS_COLS], hh.at[d, take], where, heads, "head")

    def activate(s):
        if s == 0:
            arrived(share_all.at[1:n_expert], "shares")
        table = share_all[...]
        expert = lax.broadcasted_iota(jnp.int32, table.shape, 1)
        table = jnp.sum(jnp.where(expert == me, table, 0.0), axis=1)
        table = jnp.concatenate(
            [table, jnp.zeros((LANES - n_expert, LANES), jnp.float32)], axis=0
        ).T
        for at in range(n_expert):
            kind, chip = at // chips, at % chips
            span = slice(at * rows, (at + 1) * rows)
            own_share = table[s * rows : (s + 1) * rows, at : at + 1]
            g = g_acc[span, :]
            hid[s, (kind + core + 1) % 2, chip * rows : (chip + 1) * rows, :] = (
                g / (1.0 + jnp.exp(-g)) * u_acc[span, :] * own_share
            ).astype(jnp.bfloat16)

    def down(s, i):
        j = s * n_dp + i
        if (s, i) == (0, 0):
            loaded(wd, down_sem)
        h = hid[s].reshape(n_expert * rows, hidden_w)
        for n in range(0, cols, tile):
            at = slice(n, n + tile)
            out = jnp.dot(h, wd[i, :, at], preferred_element_type=jnp.float32)
            out = out.reshape(2, chips, rows, tile)
            sb0[j, :, :, at] = out[0].astype(jnp.bfloat16)
            mine[j, :, :, at] = out[1]
        remote(sb0.at[j], rb0.at[j], to_peer, peers, (s, i, 0))

    cuts = {(subs - 1, n_dp - 2): cols // tile // 2 * tile, (subs - 1, n_dp - 1): cols - 2 * tile}

    def columns(s, i, part):
        cut = cuts.get((s, i), cols)
        return slice(cut, cols) if part else slice(0, cut)

    def both(j, chip, part, at):
        return mine[j, chip, part, at] + rb0[j, chip, part, at].astype(jnp.float32)

    def first(s, i, part=0):
        j, at = s * n_dp + i, columns(s, i, part)
        if not part:
            arrived(rb0.at[j], (s, i, 0))
        for k in range(2):
            sb1[j, 0, k, :, at] = both(j, k * 2 + 1 - xx, low, at).astype(jnp.bfloat16)
        source, target = sb1.at[j, 0, :, :, at], rb1.at[j, 0, :, :, at]
        remote(source, target, to_x, firsts, (s, i, 1, part))
        for k in range(2):
            sb1[j, 1, k, :, at] = both(j, (1 - yy) * 2 + k, high, at).astype(jnp.bfloat16)
        source, target = sb1.at[j, 1, :, :, at], rb1.at[j, 1, :, :, at]
        remote(source, target, to_y, firsts, (s, i, 2, part))

    def second(s, i, part=0):
        j, at = s * n_dp + i, columns(s, i, part)
        arrived(rb1.at[j, 0, :, :, at], (s, i, 1, part))
        out = both(j, (1 - yy) * 2 + xx, low, at) + rb1[j, 0, 1 - yy, :, at].astype(jnp.float32)
        sb2[j, 0, :, at] = out.astype(jnp.bfloat16)
        remote(sb2.at[j, 0, :, at], rb2.at[j, 0, :, at], to_y, seconds, (s, i, 3, part))
        arrived(rb1.at[j, 1, :, :, at], (s, i, 2, part))
        out = both(j, yy * 2 + 1 - xx, high, at) + rb1[j, 1, 1 - xx, :, at].astype(jnp.float32)
        sb2[j, 1, :, at] = out.astype(jnp.bfloat16)
        remote(sb2.at[j, 1, :, at], rb2.at[j, 1, :, at], to_x, seconds, (s, i, 3, part))

    def third(s, i, part=0):
        j, at = s * n_dp + i, columns(s, i, part)
        owner, mask = turns[i]
        chip = me // 2
        if i == n_dp - 1 and not part:
            arrived(rb3.at[s], (s, "over"))
        arrived(rb2.at[j, :, :, at], (s, i, 3, part))
        top = both(j, chip, low, at) + rb1[j, 0, yy, :, at].astype(jnp.float32)
        top = top + rb2[j, 0, :, at].astype(jnp.float32)
        end = both(j, chip, high, at) + rb1[j, 1, xx, :, at].astype(jnp.float32)
        end = end + rb2[j, 1, :, at].astype(jnp.float32)
        if i < n_dp - 1:
            sb3[s, i, low, at] = top.astype(jnp.bfloat16)
            sb3[s, i, high, at] = end.astype(jnp.bfloat16)
            source, target = sb3.at[s, i, :, at], rb3.at[s, mask - 1, :, at]
            remote(source, target, {"dp": owner}, thirds, (s, "over"))
        else:
            for other in range(1, n_dp):
                top = top + rb3[s, other - 1, low, at].astype(jnp.float32)
                end = end + rb3[s, other - 1, high, at].astype(jnp.float32)
            mixed_ref[s * rows : s * rows + half, at] = top.astype(jnp.bfloat16)
            mixed_ref[s * rows + half : (s + 1) * rows, at] = end.astype(jnp.bfloat16)

    def gram():
        loaded(hx.at[0], hist_sem)
        loaded(hh.at[0], head_sem)
        arrived(hx.at[1:n_dp], "hist")
        arrived(hh.at[1:n_dp], "head")
        scale = 2.0 / (n_dp * hx.shape[1])

        @pl.loop(0, cols // tile)
        def _(n):
            at = pl.multiple_of(n * tile, tile)
            left = hx[:, :, pl.ds(at, tile)].reshape(n_dp * hx.shape[1], tile)
            right = hh[...].reshape(n_dp * hx.shape[1], HESS_COLS)
            product = lax.dot_general(
                left, right, (((0,), (0,)), ((), ())), preferred_element_type=jnp.float32
            )
            hess_ref[pl.ds(at, tile), :] = product * scale

    own(0, 0)
    own(0, 1)
    own(0, 2)
    rounds(0)
    history(2)
    rounds(1)
    send_shares()
    relay(0, 0)
    own(0, 3)
    relay(0, 1)
    own(1, 0)
    relay(0, 2)
    own(1, 1)
    corner(0, 0)
    corner(0, 1)
    @pl.when(inner == 1)
    def _():
        history(3)

    widen(0, 0)
    widen(0, 1)
    relay(1, 0)
    own(1, 2)
    own(1, 3)
    corner(0, 2)
    arrive(0)
    widen(0, 2)
    relay(1, 1)
    widen(0, 3)
    corner(1, 0)
    activate(0)
    down(0, 0)
    down(0, 1)
    relay(1, 2)
    first(0, 0)
    history(1)
    down(0, 2)
    first(0, 1)
    corner(1, 1)
    widen(1, 0)
    first(0, 2)
    widen(1, 1)
    corner(1, 2)
    arrive(1)
    @pl.when(inner == 0)
    def _():
        history(3)

    widen(1, 2)
    widen(1, 3)
    second(0, 0)
    activate(1)
    down(1, 0)
    down(1, 1)
    second(0, 1)
    first(1, 0)
    down(1, 2)
    second(0, 2)
    first(1, 1)
    third(0, 0)
    down(1, 3)
    third(0, 1)
    down(0, 3)
    second(1, 0)
    first(1, 2, 0)
    first(1, 2, 1)
    third(0, 2)
    second(1, 1)
    third(1, 0)
    first(0, 3)
    gram()
    second(1, 2, 0)
    second(1, 2, 1)
    third(1, 1)
    first(1, 3, 0)
    first(1, 3, 1)
    second(0, 3)
    third(1, 2, 0)
    third(1, 2, 1)
    second(1, 3, 0)
    second(1, 3, 1)
    third(0, 3)
    third(1, 3, 0)
    third(1, 3, 1)
    departed(mine.at[0 : mine.shape[0] - 1], gathers)
    departed(sb0, peers)
    departed(sb1, firsts)
    departed(sb2, seconds)
    departed(sb3, thirds)
    departed(hx.at[1:n_dp], hists)
    departed(hh.at[1:n_dp], heads)
    departed(share_all.at[1:n_expert], parts)


def store_kernel(mixed, hess, mixed_out, hess_out, sem):
    copies = [
        pltpu.make_async_copy(hess, hess_out, sem.at[0]),
        pltpu.make_async_copy(mixed, mixed_out, sem.at[1]),
    ]
    for copy in copies:
        copy.start()
    for copy in copies:
        copy.wait()


def everyone(tokens, routes, route_weight, w_gate, w_up, w_down, prev_inputs):
    total_rows, width = tokens.shape
    n_expert = lax.axis_size("expert")
    n_dp = lax.axis_size("dp")
    hidden_w = w_gate.shape[2]
    prev = prev_inputs.reshape(prev_inputs.shape[2], width)
    cols = width // n_dp
    chunks = 4
    depth = width // chunks
    chips = n_expert // 2
    rows = total_rows // SUBS
    half = rows // 2
    steps = SUBS * n_dp
    bf16, f32 = jnp.bfloat16, jnp.float32
    arrivals = SUBS * (4 * chunks - 2) + SUBS * (4 * n_dp + 1) + 3 + 2 * 3
    vmem = pl.BlockSpec(memory_space=pltpu.VMEM)
    hbm = pl.BlockSpec(memory_space=pl.ANY)
    mixed, hess = pl.pallas_call(
        functools.partial(dense_kernel, n_dp, n_expert),
        out_shape=(
            pltpu.VMEM((total_rows, cols), bf16),
            pltpu.VMEM((cols, HESS_COLS), f32),
        ),
        in_specs=[hbm] * 7,
        out_specs=(vmem, vmem),
        scratch_shapes=[
            pltpu.VMEM((SUBS, chunks, 2, chips, rows, depth), bf16),
            pltpu.VMEM((n_expert, n_expert, LANES), f32),
            pltpu.VMEM((chunks, depth, hidden_w), bf16),
            pltpu.VMEM((chunks, depth, hidden_w), bf16),
            pltpu.VMEM((n_dp, hidden_w, cols), bf16),
            pltpu.VMEM((n_expert * rows, hidden_w), f32),
            pltpu.VMEM((n_expert * rows, hidden_w), f32),
            pltpu.VMEM((SUBS, 2, chips * rows, hidden_w), bf16),
            pltpu.VMEM((steps, chips, rows, cols), f32),
            pltpu.VMEM((steps, chips, rows, cols), bf16),
            pltpu.VMEM((steps, chips, rows, cols), bf16),
            pltpu.VMEM((steps, 2, 2, half, cols), bf16),
            pltpu.VMEM((steps, 2, 2, half, cols), bf16),
            pltpu.VMEM((steps, 2, half, cols), bf16),
            pltpu.VMEM((steps, 2, half, cols), bf16),
            pltpu.VMEM((SUBS, n_dp - 1, rows, cols), bf16),
            pltpu.VMEM((SUBS, n_dp - 1, rows, cols), bf16),
            pltpu.VMEM((n_dp, prev.shape[0], cols), bf16),
            pltpu.VMEM((n_dp, prev.shape[0], HESS_COLS), bf16),
            pltpu.VMEM((routes.shape[1], total_rows), jnp.int32),
            pltpu.VMEM((routes.shape[1], total_rows), jnp.int32),
            pltpu.SemaphoreType.DMA((8,)),
            pltpu.SemaphoreType.DMA((8,)),
            pltpu.SemaphoreType.DMA((arrivals,)),
            pltpu.SemaphoreType.REGULAR((2,)),
        ],
        compiler_params=pltpu.CompilerParams(
            collective_id=0, has_side_effects=True, vmem_limit_bytes=58000000
        ),
        name="dense_layer",
    )(tokens, routes.T, route_weight.T, w_gate[0], w_up[0], w_down[0], prev)
    mixed, hess = pl.pallas_call(
        store_kernel,
        out_shape=(
            jax.ShapeDtypeStruct(mixed.shape, bf16),
            jax.ShapeDtypeStruct(hess.shape, f32),
        ),
        in_specs=[vmem] * 2,
        out_specs=(hbm, hbm),
        scratch_shapes=[pltpu.SemaphoreType.DMA((2,))],
        compiler_params=pltpu.CompilerParams(vmem_limit_bytes=4194304),
        name="store_outputs",
    )(mixed, hess)
    return mixed, hess.reshape(cols, 1, HESS_COLS)


def shards(tokens, routes, route_weight, w_gate, w_up, w_down, prev_inputs):
    n_expert = lax.axis_size("expert")
    n_dp = lax.axis_size("dp")
    if w_gate.shape[0] == 1 and routes.shape[1] == n_expert == 2 * 2 * 2 and n_dp == 2 * 2:
        return everyone(tokens, routes, route_weight, w_gate, w_up, w_down, prev_inputs)
    hessian = gram_window(prev_inputs, n_dp, tokens.shape[1])
    return slotted(tokens, routes, route_weight, w_gate, w_up, w_down), hessian


def solution(mesh):
    placed = (
        P("expert", None),
        P("expert", None),
        P("expert", None),
        P("expert", None, "dp"),
        P("expert", None, "dp"),
        P("expert", "dp", None),
        P("dp", "expert", None, None),
    )
    return jax.shard_map(
        shards,
        mesh=mesh,
        in_specs=placed,
        out_specs=(P("expert", "dp"), P("dp", "expert", None)),
        check_vma=False,
    )
```

```python
import functools

import jax
import jax.numpy as jnp
from jax import lax
from jax.experimental import pallas as pl
from jax.experimental.pallas import tpu as pltpu
from jax.sharding import PartitionSpec as P

HESS_COLS = 128


def route_slots(flat_ids, experts_all):
    onehot = (flat_ids[:, None] == jnp.arange(experts_all, dtype=jnp.int32)[None, :]).astype(
        jnp.int32
    )
    earlier = jnp.cumsum(onehot, axis=0) - onehot
    return jnp.sum(earlier * onehot, axis=1)


def combine_rows(back, places, shares, tok_dev, top):
    columns = back.shape[-1]
    rows = back.reshape(-1, columns)[places]
    weighted = rows.astype(jnp.float32) * shares.reshape(-1, 1)
    return jnp.sum(weighted.reshape(tok_dev, top, columns), axis=1)


def route_shares(route_weight):
    weight_counts = route_weight.astype(jnp.float32)
    return 2.5 * weight_counts / jnp.sum(weight_counts, axis=1, keepdims=True)


def gram_window(prev_inputs, n_dp, width):
    history = prev_inputs.reshape(prev_inputs.shape[1], prev_inputs.shape[2], width)
    head_cols = history[:, :, :HESS_COLS]
    gram_scale = 2.0 / (n_dp * history.shape[1])
    return lax.psum_scatter(
        (
            jnp.einsum("jrd,jrh->djh", history, head_cols, preferred_element_type=jnp.float32)
            * gram_scale
        ).astype(jnp.bfloat16),
        "dp",
        scatter_dimension=0,
        tiled=True,
    ).astype(jnp.float32)


def slotted(tokens, routes, route_weight, w_gate, w_up, w_down):
    tok_dev, top = routes.shape
    exp_dev = w_gate.shape[0]
    width = tokens.shape[1]
    n_expert = lax.axis_size("expert")
    experts_all = exp_dev * n_expert
    capacity = min(tok_dev, tok_dev * top * 5 // (4 * experts_all))
    flat_ids = routes.reshape(-1)
    slots = route_slots(flat_ids, experts_all)
    places = flat_ids * capacity + slots
    shares = route_shares(route_weight)
    picks = jnp.arange(experts_all * capacity, dtype=jnp.int32)[:, None] == places[None, :]
    placing = jnp.any(picks.reshape(experts_all * capacity, tok_dev, top), axis=2).astype(
        jnp.bfloat16
    )
    outgoing = jnp.dot(placing, tokens, preferred_element_type=jnp.float32).astype(jnp.bfloat16)
    outgoing = outgoing.reshape(experts_all, capacity, width)
    arrived = lax.all_to_all(outgoing, "expert", split_axis=0, concat_axis=0, tiled=True)
    arrived = arrived.reshape(n_expert, exp_dev, capacity, width)
    gate = jnp.einsum("sjcd,jdf->sjcf", arrived, w_gate, preferred_element_type=jnp.float32)
    up = jnp.einsum("sjcd,jdf->sjcf", arrived, w_up, preferred_element_type=jnp.float32)
    hidden = (jax.nn.silu(gate) * up).astype(jnp.bfloat16)
    partial_out = jnp.einsum("sjcf,jfd->sjcd", hidden, w_down, preferred_element_type=jnp.float32)
    partial_out = partial_out.astype(jnp.bfloat16)
    back = lax.all_to_all(
        partial_out.reshape(experts_all, capacity, width),
        "expert",
        split_axis=0,
        concat_axis=0,
        tiled=True,
    )
    own_sum = combine_rows(back, places, shares, tok_dev, top)
    return lax.psum_scatter(own_sum.astype(jnp.bfloat16), "dp", scatter_dimension=1, tiled=True)

LANES = 128
SUBS = 2
MESH = pl.DeviceIdType.MESH


def flip(index, bit):
    return index + bit - 2 * bit * ((index // bit) % 2)


def partner(index, mask):
    bit = 1
    while bit <= mask:
        if mask & bit:
            index = flip(index, bit)
        bit *= 2
    return index


def dense_kernel(
    n_dp,
    n_expert,
    tokens,
    routes,
    route_weight,
    w_gate,
    w_up,
    w_down,
    prev,
    mixed_ref,
    hess_ref,
    xall,
    share_all,
    wg,
    wu,
    wd,
    g_acc,
    u_acc,
    hid,
    mine,
    sb0,
    rb0,
    sb1,
    rb1,
    sb2,
    rb2,
    sb3,
    rb3,
    hx,
    hh,
    ids,
    counts,
    lsem,
    send_sem,
    recv_sem,
    round_sem,
):
    me = lax.axis_index("expert")
    my_dp = lax.axis_index("dp")
    core, xx, yy = me % 2, (me // 2) % 2, (me // 4) % 2
    peer, ex, ey = flip(me, 1), flip(me, 2), flip(me, 4)
    ed = flip(ex, 4)
    subs, chunks, depth = xall.shape[0], xall.shape[1], xall.shape[-1]
    rows = xall.shape[4]
    half = rows // 2
    chips = n_expert // 2
    cols = rb3.shape[-1]
    hidden_w = wg.shape[-1]
    to_peer, to_x, to_y = {"expert": peer}, {"expert": ex}, {"expert": ey}
    has_lower = (my_dp + n_dp - 1) // n_dp
    has_upper = (n_dp - 1 - my_dp + n_dp - 1) // n_dp

    def greet(sem):
        for where in (to_peer, to_x, to_y):
            pl.semaphore_signal(sem, inc=1, device_id=where, device_id_type=MESH)
        for exists, where in ((has_lower, my_dp - 1), (has_upper, my_dp + 1)):

            @pl.when(exists == 1)
            def _():
                pl.semaphore_signal(sem, inc=1, device_id={"dp": where}, device_id_type=MESH)

    def met(sem):
        pl.semaphore_wait(sem, 3 + has_lower + has_upper)

    def rounds(n):
        greet(round_sem.at[n])
        met(round_sem.at[n])

    barrier = pltpu.get_barrier_semaphore()
    greet(barrier)

    tokens_sem, gate_sem, up_sem, down_sem, hist_sem, head_sem, ids_sem, counts_sem = range(8)
    gathers, sums, thirds, hists, heads, parts = range(6)
    lanes = {}

    def local(src, dst, sem):
        pltpu.make_async_copy(src, dst, lsem.at[sem]).start()

    def loaded(ref, sem):
        pltpu.make_async_copy(ref, ref, lsem.at[sem]).wait()

    def describe(src, dst, where, group, key):
        return pltpu.make_async_remote_copy(
            src_ref=src,
            dst_ref=dst,
            send_sem=send_sem.at[group],
            recv_sem=recv_sem.at[lanes.setdefault(key, len(lanes))],
            device_id=where,
            device_id_type=MESH,
        )

    def remote(src, dst, where, group, key):
        describe(src, dst, where, group, key).start()

    def arrived(ref, key):
        describe(ref, ref, to_peer, 0, key).wait_recv()

    def departed(ref, group):
        describe(ref, ref, to_peer, group, (0, 0, "x")).wait_send()

    side = my_dp % 2
    last = chunks - 1

    def piece(c):
        return pl.ds(pl.multiple_of((side * last + c * (1 - 2 * side)) * depth, LANES), depth)

    for s in range(subs):
        for c in range(chunks):
            local(
                tokens.at[s * rows : (s + 1) * rows, piece(c)],
                xall.at[s, c, core, me // 2],
                tokens_sem,
            )
    local(routes, ids, ids_sem)
    local(route_weight, counts, counts_sem)
    for c in range(chunks):
        local(w_gate.at[piece(c), :], wg.at[c], gate_sem)
        local(w_up.at[piece(c), :], wu.at[c], up_sem)
    odd = my_dp % 2
    inner = (my_dp + my_dp // 2) % 2
    turns = [
        ((n_dp - 1) * (1 - my_dp // 2), 3 - inner),
        (flip(my_dp, 2) * (1 - inner) + flip(my_dp, 1) * inner, 2 - inner),
        (1 + odd, 1 + 2 * inner),
        (my_dp, 0),
    ]
    for i, (owner, _) in enumerate(turns):
        start = pl.multiple_of(owner * cols, LANES)
        local(w_down.at[:, pl.ds(start, cols)], wd.at[i], down_sem)
    local(prev.at[:, pl.ds(pl.multiple_of(my_dp * cols, LANES), cols)], hx.at[0], hist_sem)
    local(prev.at[:, 0:HESS_COLS], hh.at[0], head_sem)

    met(barrier)

    to_z = {"dp": flip(my_dp, 1)}

    def block(s, c, who):
        return xall.at[s, c, who % 2, who // 2]

    def own(s, c):
        if (s, c) == (0, 0):
            loaded(tokens, tokens_sem)
        here = block(s, c, me)
        if c < last:
            remote(here, here, to_x, gathers, (s, c, "x"))
            remote(here, here, to_y, gathers, (s, c, "y"))
        remote(here, here, to_peer, gathers, (s, c, "p"))

    def share_block(s, c, who):
        remote(block(s, c, who), block(s, c, who), to_peer, gathers, (s, c, "p"))

    def across(s, who):
        remote(block(s, 0, who), block(s, last, who), to_z, gathers, (s, "z"))

    low, high = slice(0, half), slice(half, rows)

    def relay(s, c):
        for name, who, forth, part in (("x", ex, to_y, low), ("y", ey, to_x, high)):
            here = block(s, c, who)
            arrived(here, (s, c, name))
            remote(here.at[part], here.at[part], forth, gathers, (s, c, "d"))
            if c == 0:
                across(s, who)
            share_block(s, c, who)

    def corner(s, c):
        arrived(block(s, c, ed), (s, c, "d"))
        if c == 0:
            across(s, ed)
        share_block(s, c, ed)

    def arrive(s):
        arrived(xall.at[s, last, core, 1:chips], (s, "z"))
        for who in (ex, ey, ed):
            share_block(s, last, who)

    tile = 2 * LANES

    def widen(s, c):
        arrived(xall.at[s, c, 1 - core], (s, c, "p"))
        if (s, c) == (0, 0):
            loaded(wg, gate_sem)
            loaded(wu, up_sem)
        x = xall[s, c].reshape(n_expert * rows, depth)
        for n in range(0, hidden_w, tile):
            at = slice(n, n + tile)
            g = jnp.dot(x, wg[c, :, at], preferred_element_type=jnp.float32)
            u = jnp.dot(x, wu[c, :, at], preferred_element_type=jnp.float32)
            if c == 0:
                g_acc[:, at] = g
                u_acc[:, at] = u
            else:
                g_acc[:, at] += g
                u_acc[:, at] += u

    def send_shares():
        loaded(ids, ids_sem)
        loaded(counts, counts_sem)
        weight = counts[...].astype(jnp.float32)
        part = 2.5 * weight / jnp.sum(weight, axis=0, keepdims=True)
        named = ids[...]
        expert = lax.broadcasted_iota(jnp.int32, (n_expert, named.shape[1]), 0)
        by_expert = jnp.zeros(expert.shape, jnp.float32)
        for k in range(named.shape[0]):
            by_expert += jnp.where(named[k : k + 1, :] == expert, part[k : k + 1, :], 0.0)
        here = share_all.at[core * chips + me // 2]
        here[...] = jnp.zeros((n_expert, LANES), jnp.float32)
        here[:, 0 : named.shape[1]] = by_expert
        for d in range(1, n_expert):
            remote(here, here, {"expert": (me + d) % n_expert}, parts, "shares")

    def history(d, first_half=True, second_half=True):
        count = hx.shape[1]
        take = slice(0 if first_half else count // 2, count if second_half else count // 2)
        start = pl.multiple_of(partner(my_dp, d) * cols, LANES)
        where = {"dp": partner(my_dp, d)}
        remote(prev.at[take, pl.ds(start, cols)], hx.at[d, take], where, hists, "hist")
        remote(prev.at[take, 0:HESS_COLS], hh.at[d, take], where, heads, "head")

    def activate(s):
        if s == 0:
            arrived(share_all.at[1:n_expert], "shares")
        table = share_all[...]
        expert = lax.broadcasted_iota(jnp.int32, table.shape, 1)
        table = jnp.sum(jnp.where(expert == me, table, 0.0), axis=1)
        table = jnp.concatenate(
            [table, jnp.zeros((LANES - n_expert, LANES), jnp.float32)], axis=0
        ).T
        for at in range(n_expert):
            kind, chip = at // chips, at % chips
            span = slice(at * rows, (at + 1) * rows)
            own_share = table[s * rows : (s + 1) * rows, at : at + 1]
            g = g_acc[span, :]
            hid[s, (kind + core + 1) % 2, chip * rows : (chip + 1) * rows, :] = (
                g / (1.0 + jnp.exp(-g)) * u_acc[span, :] * own_share
            ).astype(jnp.bfloat16)

    def down(s, i):
        j = s * n_dp + i
        if (s, i) == (0, 0):
            loaded(wd, down_sem)
        h = hid[s].reshape(n_expert * rows, hidden_w)
        for n in range(0, cols, tile):
            at = slice(n, n + tile)
            out = jnp.dot(h, wd[i, :, at], preferred_element_type=jnp.float32)
            out = out.reshape(2, chips, rows, tile)
            sb0[j, :, :, at] = out[0].astype(jnp.bfloat16)
            mine[j, :, :, at] = out[1]
        remote(sb0.at[j], rb0.at[j], to_peer, sums, (s, i, 0))

    middle = cols // tile // 2 * tile
    cuts = {(s, n_dp - 2): middle for s in range(subs)}
    cuts[subs - 1, n_dp - 1] = cols - 2 * tile

    def columns(s, i, part):
        cut = cuts.get((s, i), cols)
        return slice(cut, cols) if part else slice(0, cut)

    def both(j, chip, part, at):
        return mine[j, chip, part, at] + rb0[j, chip, part, at].astype(jnp.float32)

    def first(s, i, part=0):
        j, at = s * n_dp + i, columns(s, i, part)
        if not part:
            arrived(rb0.at[j], (s, i, 0))
        for k in range(2):
            sb1[j, 0, k, :, at] = both(j, k * 2 + 1 - xx, low, at).astype(jnp.bfloat16)
        source, target = sb1.at[j, 0, :, :, at], rb1.at[j, 0, :, :, at]
        remote(source, target, to_x, sums, (s, i, 1, part))
        for k in range(2):
            sb1[j, 1, k, :, at] = both(j, (1 - yy) * 2 + k, high, at).astype(jnp.bfloat16)
        source, target = sb1.at[j, 1, :, :, at], rb1.at[j, 1, :, :, at]
        remote(source, target, to_y, sums, (s, i, 2, part))

    def second(s, i, part=0):
        j, at = s * n_dp + i, columns(s, i, part)
        arrived(rb1.at[j, 0, :, :, at], (s, i, 1, part))
        out = both(j, (1 - yy) * 2 + xx, low, at) + rb1[j, 0, 1 - yy, :, at].astype(jnp.float32)
        sb2[j, 0, :, at] = out.astype(jnp.bfloat16)
        remote(sb2.at[j, 0, :, at], rb2.at[j, 0, :, at], to_y, sums, (s, i, 3, part))
        arrived(rb1.at[j, 1, :, :, at], (s, i, 2, part))
        out = both(j, yy * 2 + 1 - xx, high, at) + rb1[j, 1, 1 - xx, :, at].astype(jnp.float32)
        sb2[j, 1, :, at] = out.astype(jnp.bfloat16)
        remote(sb2.at[j, 1, :, at], rb2.at[j, 1, :, at], to_x, sums, (s, i, 3, part))

    def third(s, i, part=0):
        j, at = s * n_dp + i, columns(s, i, part)
        owner, mask = turns[i]
        chip = me // 2
        if i == n_dp - 1 and not part:
            arrived(rb3.at[s], (s, "over"))
        arrived(rb2.at[j, :, :, at], (s, i, 3, part))
        top = both(j, chip, low, at) + rb1[j, 0, yy, :, at].astype(jnp.float32)
        top = top + rb2[j, 0, :, at].astype(jnp.float32)
        end = both(j, chip, high, at) + rb1[j, 1, xx, :, at].astype(jnp.float32)
        end = end + rb2[j, 1, :, at].astype(jnp.float32)
        if i < n_dp - 1:
            sb3[s, i, low, at] = top.astype(jnp.bfloat16)
            sb3[s, i, high, at] = end.astype(jnp.bfloat16)
            source, target = sb3.at[s, i, :, at], rb3.at[s, mask - 1, :, at]
            remote(source, target, {"dp": owner}, thirds, (s, "over"))
        else:
            for other in range(1, n_dp):
                top = top + rb3[s, other - 1, low, at].astype(jnp.float32)
                end = end + rb3[s, other - 1, high, at].astype(jnp.float32)
            mixed_ref[s * rows : s * rows + half, at] = top.astype(jnp.bfloat16)
            mixed_ref[s * rows + half : (s + 1) * rows, at] = end.astype(jnp.bfloat16)

    def gram():
        loaded(hx.at[0], hist_sem)
        loaded(hh.at[0], head_sem)
        arrived(hx.at[1:n_dp], "hist")
        arrived(hh.at[1:n_dp], "head")
        scale = 2.0 / (n_dp * hx.shape[1])

        @pl.loop(0, cols // tile)
        def _(n):
            at = pl.multiple_of(n * tile, tile)
            left = hx[:, :, pl.ds(at, tile)].reshape(n_dp * hx.shape[1], tile)
            right = hh[...].reshape(n_dp * hx.shape[1], HESS_COLS)
            product = lax.dot_general(
                left, right, (((0,), (0,)), ((), ())), preferred_element_type=jnp.float32
            )
            hess_ref[pl.ds(at, tile), :] = product * scale

    own(0, 0)
    own(0, 1)
    own(0, 2)
    rounds(0)
    history(2)
    rounds(1)
    send_shares()
    relay(0, 0)
    own(0, 3)
    relay(0, 1)
    own(1, 0)
    relay(0, 2)
    own(1, 1)
    corner(0, 0)
    corner(0, 1)
    @pl.when(inner == 1)
    def _():
        history(3)

    widen(0, 0)
    widen(0, 1)
    relay(1, 0)
    own(1, 2)
    own(1, 3)
    corner(0, 2)
    arrive(0)
    widen(0, 2)
    relay(1, 1)
    widen(0, 3)
    corner(1, 0)
    activate(0)
    down(0, 0)
    down(0, 1)
    relay(1, 2)
    first(0, 0)
    history(1)
    down(0, 2)
    first(0, 1)
    corner(1, 1)
    widen(1, 0)
    first(0, 2, 0)
    widen(1, 1)
    corner(1, 2)
    arrive(1)
    @pl.when(inner == 0)
    def _():
        history(3)

    widen(1, 2)
    second(0, 0)
    first(0, 2, 1)
    widen(1, 3)
    activate(1)
    down(1, 0)
    down(1, 1)
    second(0, 1)
    first(1, 0)
    third(0, 0)
    down(1, 2)
    second(0, 2, 0)
    second(0, 2, 1)
    first(1, 1)
    third(0, 1)
    down(1, 3)
    down(0, 3)
    second(1, 0)
    first(1, 2, 0)
    first(1, 2, 1)
    third(0, 2, 0)
    third(0, 2, 1)
    second(1, 1)
    third(1, 0)
    first(0, 3)
    gram()
    second(1, 2, 0)
    second(1, 2, 1)
    third(1, 1)
    first(1, 3, 0)
    first(1, 3, 1)
    second(0, 3)
    third(1, 2, 0)
    third(1, 2, 1)
    second(1, 3, 0)
    second(1, 3, 1)
    third(0, 3)
    third(1, 3, 0)
    third(1, 3, 1)
    departed(mine.at[0 : mine.shape[0] - 1], gathers)
    departed(mine.at[0 : mine.shape[0] - 1], sums)
    departed(sb3, thirds)
    departed(hx.at[1:n_dp], hists)
    departed(hh.at[1:n_dp], heads)
    departed(share_all.at[1:n_expert], parts)


def store_kernel(mixed, hess, mixed_out, hess_out, sem):
    copies = [
        pltpu.make_async_copy(hess, hess_out, sem.at[0]),
        pltpu.make_async_copy(mixed, mixed_out, sem.at[1]),
    ]
    for copy in copies:
        copy.start()
    for copy in copies:
        copy.wait()


def everyone(tokens, routes, route_weight, w_gate, w_up, w_down, prev_inputs):
    total_rows, width = tokens.shape
    n_expert = lax.axis_size("expert")
    n_dp = lax.axis_size("dp")
    hidden_w = w_gate.shape[2]
    prev = prev_inputs.reshape(prev_inputs.shape[2], width)
    cols = width // n_dp
    chunks = 4
    depth = width // chunks
    chips = n_expert // 2
    rows = total_rows // SUBS
    half = rows // 2
    steps = SUBS * n_dp
    bf16, f32 = jnp.bfloat16, jnp.float32
    arrivals = SUBS * (4 * chunks - 2) + SUBS * (4 * n_dp + 1) + 3 + 3 * 3
    vmem = pl.BlockSpec(memory_space=pltpu.VMEM)
    hbm = pl.BlockSpec(memory_space=pl.ANY)
    mixed, hess = pl.pallas_call(
        functools.partial(dense_kernel, n_dp, n_expert),
        out_shape=(
            pltpu.VMEM((total_rows, cols), bf16),
            pltpu.VMEM((cols, HESS_COLS), f32),
        ),
        in_specs=[hbm] * 7,
        out_specs=(vmem, vmem),
        scratch_shapes=[
            pltpu.VMEM((SUBS, chunks, 2, chips, rows, depth), bf16),
            pltpu.VMEM((n_expert, n_expert, LANES), f32),
            pltpu.VMEM((chunks, depth, hidden_w), bf16),
            pltpu.VMEM((chunks, depth, hidden_w), bf16),
            pltpu.VMEM((n_dp, hidden_w, cols), bf16),
            pltpu.VMEM((n_expert * rows, hidden_w), f32),
            pltpu.VMEM((n_expert * rows, hidden_w), f32),
            pltpu.VMEM((SUBS, 2, chips * rows, hidden_w), bf16),
            pltpu.VMEM((steps, chips, rows, cols), f32),
            pltpu.VMEM((steps, chips, rows, cols), bf16),
            pltpu.VMEM((steps, chips, rows, cols), bf16),
            pltpu.VMEM((steps, 2, 2, half, cols), bf16),
            pltpu.VMEM((steps, 2, 2, half, cols), bf16),
            pltpu.VMEM((steps, 2, half, cols), bf16),
            pltpu.VMEM((steps, 2, half, cols), bf16),
            pltpu.VMEM((SUBS, n_dp - 1, rows, cols), bf16),
            pltpu.VMEM((SUBS, n_dp - 1, rows, cols), bf16),
            pltpu.VMEM((n_dp, prev.shape[0], cols), bf16),
            pltpu.VMEM((n_dp, prev.shape[0], HESS_COLS), bf16),
            pltpu.VMEM((routes.shape[1], total_rows), jnp.int32),
            pltpu.VMEM((routes.shape[1], total_rows), jnp.int32),
            pltpu.SemaphoreType.DMA((8,)),
            pltpu.SemaphoreType.DMA((6,)),
            pltpu.SemaphoreType.DMA((arrivals,)),
            pltpu.SemaphoreType.REGULAR((2,)),
        ],
        compiler_params=pltpu.CompilerParams(
            collective_id=0, has_side_effects=True, vmem_limit_bytes=58000000
        ),
        name="dense_layer",
    )(tokens, routes.T, route_weight.T, w_gate[0], w_up[0], w_down[0], prev)
    mixed, hess = pl.pallas_call(
        store_kernel,
        out_shape=(
            jax.ShapeDtypeStruct(mixed.shape, bf16),
            jax.ShapeDtypeStruct(hess.shape, f32),
        ),
        in_specs=[vmem] * 2,
        out_specs=(hbm, hbm),
        scratch_shapes=[pltpu.SemaphoreType.DMA((2,))],
        compiler_params=pltpu.CompilerParams(vmem_limit_bytes=4194304),
        name="store_outputs",
    )(mixed, hess)
    return mixed, hess.reshape(cols, 1, HESS_COLS)


def shards(tokens, routes, route_weight, w_gate, w_up, w_down, prev_inputs):
    n_expert = lax.axis_size("expert")
    n_dp = lax.axis_size("dp")
    if w_gate.shape[0] == 1 and routes.shape[1] == n_expert == 2 * 2 * 2 and n_dp == 2 * 2:
        return everyone(tokens, routes, route_weight, w_gate, w_up, w_down, prev_inputs)
    hessian = gram_window(prev_inputs, n_dp, tokens.shape[1])
    return slotted(tokens, routes, route_weight, w_gate, w_up, w_down), hessian


def solution(mesh):
    placed = (
        P("expert", None),
        P("expert", None),
        P("expert", None),
        P("expert", None, "dp"),
        P("expert", None, "dp"),
        P("expert", "dp", None),
        P("dp", "expert", None, None),
    )
    return jax.shard_map(
        shards,
        mesh=mesh,
        in_specs=placed,
        out_specs=(P("expert", "dp"), P("dp", "expert", None)),
        check_vma=False,
    )
```
